32 devices in a mesh: gx: 4 (over y, core), gz: 2 (over x), ta: 4 (over z).
Axes of the slice: x: 2, y: 2, z: 4, core: 2. Of those that a mesh axis runs over, the one named last changes fastest.
Arguments:
- links: float32 [4, 2, 3, 3, 16, 8, 512], P(None, None, None, None, 'ta', 'gz', 'gx'), may hold values from -1 to 1, as said below
Outputs:
- force: float32 [4, 2, 3, 3, 16, 8, 512], P(None, None, None, None, 'ta', 'gz', 'gx')
The draws below stay inside these ranges and needn't reach their ends.
Inputs may be any that keep to these rules, and one draw needn't show every extreme that they name: Every link matrix (real part links[mu, 0], imaginary part links[mu, 1]) is special unitary, up to float32 rounding.
All inputs are finite; a program needn't handle non-finite values.
Results may differ from the reference program's by a relative error of at most 0.0003.
Values sent between devices are 32-bit elements; how exact they have to be, the bound alone decides.
A program may use at most 64 MiB of HBM per device.

```python
import jax
import jax.numpy as jnp

NX = 16
NY = 32
NZ = 8
NT = 16
NXY = 512


def draw_links(key, part):
    sample = jax.random.normal(key, (2, 4, 3, 3, NT, NZ, NXY), jnp.float32)
    real0 = sample[0][:, 0]
    imag0 = sample[1][:, 0]
    length0 = jnp.maximum(jnp.sqrt(jnp.sum(real0 * real0 + imag0 * imag0, axis=1, keepdims=True)), 1e-06)
    real0 = real0 / length0
    imag0 = imag0 / length0
    real1 = sample[0][:, 1]
    imag1 = sample[1][:, 1]
    inner_real = jnp.sum(real0 * real1 + imag0 * imag1, axis=1, keepdims=True)
    inner_imag = jnp.sum(real0 * imag1 - imag0 * real1, axis=1, keepdims=True)
    real1 = real1 - (inner_real * real0 - inner_imag * imag0)
    imag1 = imag1 - (inner_real * imag0 + inner_imag * real0)
    length1 = jnp.maximum(jnp.sqrt(jnp.sum(real1 * real1 + imag1 * imag1, axis=1, keepdims=True)), 1e-06)
    real1 = real1 / length1
    imag1 = imag1 / length1
    real_cols = []
    imag_cols = []
    for column in range(3):
        next_col = (column + 1) % 3
        last_col = (column + 2) % 3
        cross_real = real0[:, next_col] * real1[:, last_col] - imag0[:, next_col] * imag1[:, last_col] - real0[:, last_col] * real1[:, next_col] + imag0[:, last_col] * imag1[:, next_col]
        cross_imag = real0[:, next_col] * imag1[:, last_col] + imag0[:, next_col] * real1[:, last_col] - real0[:, last_col] * imag1[:, next_col] - imag0[:, last_col] * real1[:, next_col]
        real_cols.append(cross_real)
        imag_cols.append(-cross_imag)
    real2 = jnp.stack(real_cols, axis=1)
    imag2 = jnp.stack(imag_cols, axis=1)
    real_rows = jnp.stack([real0, real1, real2], axis=1)
    imag_rows = jnp.stack([imag0, imag1, imag2], axis=1)
    return jnp.stack([real_rows, imag_rows], axis=1)


def setup_inputs(seed: int = 0) -> dict:
    seeds = jax.random.split(jax.random.key(seed), 2)
    links = draw_links(jax.random.fold_in(seeds[1], 71), 0)
    return dict(links=links)


COEFF = -1.9


def matprod(left, right):
    total = left[:, 0][:, None] * right[0][None, :]
    total = total + left[:, 1][:, None] * right[1][None, :]
    return total + left[:, 2][:, None] * right[2][None, :]


def complex_mul(left, right):
    return (matprod(left[0], right[0]) - matprod(left[1], right[1]),
            matprod(left[0], right[1]) + matprod(left[1], right[0]))


def dagger(matrix):
    return (jnp.swapaxes(matrix[0], 0, 1), -jnp.swapaxes(matrix[1], 0, 1))


def unit_step(direction, sign):
    offset = [0, 0, 0, 0]
    offset[direction] = sign
    return tuple(offset)


def joined(first_step, second_step):
    return tuple(first_step[position] + second_step[position] for position in range(4))


def gauge_force(fetch_link):
    blocks = []
    still = (0, 0, 0, 0)
    for direction in range(4):
        ahead = unit_step(direction, 1)
        summed = None
        for transverse in range(4):
            if transverse == direction:
                continue
            side_up = unit_step(transverse, 1)
            side_down = unit_step(transverse, -1)
            upper = complex_mul(complex_mul(fetch_link(transverse, ahead), dagger(fetch_link(direction, side_up))),
                                dagger(fetch_link(transverse, still)))
            lower = complex_mul(complex_mul(dagger(fetch_link(transverse, joined(ahead, side_down))),
                                            dagger(fetch_link(direction, side_down))),
                                fetch_link(transverse, side_down))
            staple = (upper[0] + lower[0], upper[1] + lower[1])
            summed = staple if summed is None else (summed[0] + staple[0], summed[1] + staple[1])
        loop_matrix = complex_mul(fetch_link(direction, still), summed)
        real_part = 0.5 * (loop_matrix[0] - jnp.swapaxes(loop_matrix[0], 0, 1))
        imag_part = 0.5 * (loop_matrix[1] + jnp.swapaxes(loop_matrix[1], 0, 1))
        trace_third = (loop_matrix[1][0, 0] + loop_matrix[1][1, 1] + loop_matrix[1][2, 2]) / 3.0
        identity = jnp.eye(3, dtype=jnp.float32).reshape((3, 3) + (1,) * trace_third.ndim)
        imag_part = imag_part - identity * trace_third
        blocks.append(COEFF * jnp.stack([real_part, imag_part], axis=0))
    return jnp.stack(blocks, axis=0)


def reference(links):
    lattice = links.reshape(links.shape[:6] + (NY, NX))

    def fetch_link(direction, offset):
        field = lattice[direction]
        field = jnp.roll(field, (-offset[0], -offset[1], -offset[2], -offset[3]), axis=(3, 4, 5, 6))
        return (field[0], field[1])

    return gauge_force(fetch_link).reshape(links.shape)
```

```python
import functools

import jax
import jax.numpy as jnp
from jax import lax
from jax.experimental import pallas as pl
from jax.experimental.pallas import tpu as pltpu
from jax.sharding import PartitionSpec as P

NX = 16
COEFF = -1.9
AXES = ("ta", "gz", "gx")
SUB, LANES = 8, 128


def others(d):
    return [m for m in range(4) if m != d]


class Lattice:
    def __init__(self, depth):
        self.depth = depth
        self.per = SUB // depth
        self.ygroups = LANES // NX
        self.row = lax.broadcasted_iota(jnp.int32, (SUB, LANES), 0)
        self.lane = lax.broadcasted_iota(jnp.int32, (SUB, LANES), 1)
        self.zrow = self.row % depth
        self.xcol = self.lane % NX

    def rows(self, value, shift):
        shift %= SUB
        return pltpu.roll(value, shift, 0) if shift else value

    def lanes(self, value, shift):
        shift %= LANES
        return pltpu.roll(value, shift, 1) if shift else value


def entry(left, right, i, j, part, left_h, right_h):
    total = None
    for k in range(3):
        li = (k, i) if left_h else (i, k)
        ri = (j, k) if right_h else (k, j)
        lr, lm = left[0][li[0]][li[1]], left[1][li[0]][li[1]]
        rr, rm = right[0][ri[0]][ri[1]], right[1][ri[0]][ri[1]]
        if part == 0:
            first, second = lr * rr, lm * rm
            minus = left_h == right_h
        elif left_h:
            first, second = lr * rm, lm * rr
            minus = True
        else:
            first, second = lm * rr, lr * rm
            minus = right_h
        value = first - second if minus else first + second
        total = value if total is None else total + value
    return total


def product(left, right, left_h=False, right_h=False):
    return [
        [[entry(left, right, i, j, part, left_h, right_h) for j in range(3)] for i in range(3)]
        for part in range(2)
    ]


def projected(left, right, left_h=False, right_h=False):
    get = lambda i, j, part: entry(left, right, i, j, part, left_h, right_h)
    pairs = ((0, 1), (0, 2), (1, 2))
    real = [get(i, j, 0) - get(j, i, 0) for i, j in pairs]
    imag = [get(i, j, 1) + get(j, i, 1) for i, j in pairs]
    diag = [get(i, i, 1) for i in range(3)]
    third = (diag[0] + diag[1] + diag[2]) * (1.0 / 3.0)
    return real + imag + [diag[0] - third, diag[1] - third]


def third_row(real, imag):
    rows_r, rows_i = [], []
    for column in range(3):
        n, l = (column + 1) % 3, (column + 2) % 3
        rows_r.append(
            real[0][n] * real[1][l]
            - imag[0][n] * imag[1][l]
            - real[0][l] * real[1][n]
            + imag[0][l] * imag[1][n]
        )
        rows_i.append(
            real[0][l] * imag[1][n]
            + imag[0][l] * real[1][n]
            - real[0][n] * imag[1][l]
            - imag[0][n] * real[1][l]
        )
    return rows_r, rows_i


def sizes(depth, halves):
    yg = LANES // NX
    per = SUB // depth

    def rows(count):
        return (
            -(-count // per) * SUB,
            -(-count // depth) * SUB * halves,
            -(-count // yg) * SUB * halves,
        )

    return rows(36), rows(24)


def kernel(
    counts, depth, halves, u, out,
    st, sz, sy, rt, rz, ry, qt, qz, qy, pt, pz, py, acc, send, recv,
):
    g = Lattice(depth)
    me = [lax.axis_index(a) for a in AXES]
    nxt = [lax.rem(me[i] + 1, counts[i]) for i in range(3)]
    prv = [lax.rem(me[i] + counts[i] - 1, counts[i]) for i in range(3)]

    def device(i, index):
        where = list(me)
        where[i] = index
        by = dict(zip(AXES, where))
        return (by["gx"], by["gz"], by["ta"])

    barrier = pltpu.get_barrier_semaphore()
    for i in range(3):
        for index in (nxt[i], prv[i]):
            pl.semaphore_signal(
                barrier, inc=1, device_id=device(i, index), device_id_type=pl.DeviceIdType.MESH
            )

    def load(m, part, i, j, h):
        return u[m, part, i, j, h * SUB : (h + 1) * SUB, :]

    def comps(d):
        return [(m, part, i, j) for m in others(d) for part in range(2) for i in range(2) for j in range(3)]

    cs = comps(0)
    for c0 in range(0, len(cs), g.per):
        value = None
        for k in range(g.per):
            x = g.rows(load(*cs[c0 + k], 0), depth * k)
            value = x if value is None else jnp.where(g.row >= depth * k, x, value)
        st[c0 // g.per * SUB : (c0 // g.per + 1) * SUB, :] = value
    cs = comps(1)
    for c0 in range(0, len(cs), depth):
        for h in range(halves):
            value = None
            for k in range(depth):
                x = g.rows(load(*cs[c0 + k], h), k)
                value = x if value is None else jnp.where(g.zrow >= k, x, value)
            r = (c0 // depth * halves + h) * SUB
            sz[r : r + SUB, :] = value
    cs = comps(2)
    for c0 in range(0, len(cs), g.ygroups):
        for h in range(halves):
            value = None
            for k in range(min(g.ygroups, len(cs) - c0)):
                x = g.lanes(load(*cs[c0 + k], h), NX * k)
                value = x if value is None else jnp.where(g.lane >= NX * k, x, value)
            r = (c0 // g.ygroups * halves + h) * SUB
            sy[r : r + SUB, :] = value

    pl.semaphore_wait(barrier, 6)

    def remote(src, dst, slot, i, index):
        return pltpu.make_async_remote_copy(
            src_ref=src, dst_ref=dst, send_sem=send.at[slot], recv_sem=recv.at[slot],
            device_id=device(i, index), device_id_type=pl.DeviceIdType.MESH,
        )

    first = [
        remote(st, rt, 0, 0, prv[0]),
        remote(sz, rz, 1, 1, prv[1]),
        remote(sy, ry, 2, 2, prv[2]),
    ]
    second = [
        remote(qt, pt, 3, 0, nxt[0]),
        remote(qz, pz, 4, 1, nxt[1]),
        remote(qy, py, 5, 2, nxt[2]),
    ]
    for copy in first:
        copy.start()

    def matrix(m, h):
        return [[[load(m, part, i, j, h) for j in range(3)] for i in range(3)] for part in range(2)]

    def ahead(m, d, h):
        index = {c: n for n, c in enumerate(comps(d))} if d < 3 else None

        def get(part, i, j):
            v = load(m, part, i, j, h)
            if d == 3:
                return jnp.where(g.xcol == NX - 1, g.lanes(v, NX - 1), g.lanes(v, -1))
            c = index[(m, part, i, j)]
            if d == 0:
                if h + 1 < halves:
                    beyond = g.rows(load(m, part, i, j, h + 1), -depth)
                else:
                    r = c // g.per * SUB
                    beyond = g.rows(rt[r : r + SUB, :], SUB - depth - depth * (c % g.per))
                return jnp.where(g.row >= SUB - depth, beyond, g.rows(v, -depth))
            if d == 1:
                r = (c // depth * halves + h) * SUB
                edge = g.rows(rz[r : r + SUB, :], depth - 1 - c % depth)
                return jnp.where(g.zrow == depth - 1, edge, g.rows(v, -1))
            r = (c // g.ygroups * halves + h) * SUB
            edge = g.lanes(ry[r : r + SUB, :], LANES - NX - NX * (c % g.ygroups))
            return jnp.where(g.lane >= LANES - NX, edge, g.lanes(v, -NX))

        known = 3 if d == 3 else 2
        real = [[get(0, i, j) for j in range(3)] for i in range(known)]
        imag = [[get(1, i, j) for j in range(3)] for i in range(known)]
        if known == 2:
            third_r, third_i = third_row(real, imag)
            real.append(third_r)
            imag.append(third_i)
        return [real, imag]

    seen = set()

    def add(m, c, h, value):
        r = ((m * 8 + c) * halves + h) * SUB
        if (m, c, h) in seen:
            acc[r : r + SUB, :] += value
        else:
            seen.add((m, c, h))
            acc[r : r + SUB, :] = value

    def lower(m, d, h, q):
        base = others(d).index(m) * 8
        if d == 3:
            for c in range(8):
                add(m, c, h, jnp.where(g.xcol == 0, g.lanes(q[c], 1 - NX), g.lanes(q[c], 1)))
        elif d == 2:
            for c in range(8):
                add(m, c, h, jnp.where(g.lane >= NX, g.lanes(q[c], NX), 0.0))
            for c0 in range(0, 8, g.ygroups):
                value = None
                for k in range(g.ygroups):
                    x = g.lanes(q[c0 + k], NX * (k + 1))
                    value = x if value is None else jnp.where(g.lane >= NX * k, x, value)
                r = ((base + c0) // g.ygroups * halves + h) * SUB
                qy[r : r + SUB, :] = value
        elif d == 1:
            for c in range(8):
                add(m, c, h, jnp.where(g.zrow > 0, g.rows(q[c], 1), 0.0))
            for c0 in range(0, 8, depth):
                value = None
                for k in range(depth):
                    x = g.rows(q[c0 + k], k + 1 - depth)
                    value = x if value is None else jnp.where(g.zrow >= k, x, value)
                r = ((base + c0) // depth * halves + h) * SUB
                qz[r : r + SUB, :] = value
        else:
            for c in range(8):
                moved = g.rows(q[c], depth)
                add(m, c, h, jnp.where(g.row >= depth, moved, 0.0))
                if h + 1 < halves:
                    add(m, c, h + 1, jnp.where(g.row < depth, moved, 0.0))
            if h + 1 == halves:
                for c0 in range(0, 8, g.per):
                    value = None
                    for k in range(g.per):
                        x = g.rows(q[c0 + k], depth * (k + 1))
                        value = x if value is None else jnp.where(g.row >= depth * k, x, value)
                    r = (base + c0) // g.per * SUB
                    qt[r : r + SUB, :] = value

    def plane(mu, nu, h):
        here_mu, here_nu = matrix(mu, h), matrix(nu, h)
        a = product(ahead(nu, mu, h), ahead(mu, nu, h), right_h=True)
        e = product(here_mu, a)
        upper = projected(e, here_nu, right_h=True)
        for c in range(8):
            add(mu, c, h, upper[c])
            add(nu, c, h, -upper[c])
        lower(mu, nu, h, projected(e, here_nu, left_h=True))
        c_matrix = product(a, here_nu, right_h=True)
        lower(nu, mu, h, projected(c_matrix, here_mu))

    waits = {(0, 3): [0], (0, 1): [1], (0, 2): [2]}
    starts = {(0, 2): [0], (1, 2): [1], (2, 3): [2]}
    for pair in ((0, 3), (0, 1), (0, 2), (1, 3), (1, 2), (2, 3)):
        for h in range(halves):
            if h == (halves - 1 if pair == (0, 3) else 0):
                for i in waits.get(pair, ()):
                    first[i].wait_recv()
            plane(pair[0], pair[1], h)
        for i in starts.get(pair, ()):
            second[i].start()

    for copy in second:
        copy.wait_recv()
    for m in range(4):
        for h in range(halves):
            f = []
            for c in range(8):
                r = ((m * 8 + c) * halves + h) * SUB
                value = acc[r : r + SUB, :]
                for d in others(m):
                    b = others(d).index(m) * 8 + c
                    if d == 0 and h == 0:
                        r = b // g.per * SUB
                        x = g.rows(pt[r : r + SUB, :], -depth * (b % g.per))
                        value = value + jnp.where(g.row < depth, x, 0.0)
                    elif d == 1:
                        r = (b // depth * halves + h) * SUB
                        x = g.rows(pz[r : r + SUB, :], -(b % depth))
                        value = value + jnp.where(g.zrow == 0, x, 0.0)
                    elif d == 2:
                        r = (b // g.ygroups * halves + h) * SUB
                        x = g.lanes(py[r : r + SUB, :], -NX * (b % g.ygroups))
                        value = value + jnp.where(g.lane < NX, x, 0.0)
                f.append(value * (COEFF * 0.5 if c < 6 else COEFF))

            def put(part, i, j, value):
                out[m, part, i, j, h * SUB : (h + 1) * SUB, :] = value

            for n, (i, j) in enumerate(((0, 1), (0, 2), (1, 2))):
                put(0, i, j, f[n])
                put(0, j, i, -f[n])
                put(1, i, j, f[3 + n])
                put(1, j, i, f[3 + n])
            for i in range(3):
                put(0, i, i, jnp.zeros((SUB, LANES), jnp.float32))
            put(1, 0, 0, f[6])
            put(1, 1, 1, f[7])
            put(1, 2, 2, -(f[6] + f[7]))
    for copy in first + second:
        copy.wait_send()


def per_device(counts, links):
    time_len, depth, flat = links.shape[4:]
    sites = time_len * depth
    assert flat == LANES and SUB % depth == 0 and sites % SUB == 0
    halves = sites // SUB
    rows1, rows2 = sizes(depth, halves)
    vmem = lambda r: pltpu.VMEM((r, LANES), jnp.float32)
    shape = links.shape[:4] + (sites, flat)
    out = pl.pallas_call(
        functools.partial(kernel, counts, depth, halves),
        out_shape=jax.ShapeDtypeStruct(shape, jnp.float32),
        in_specs=[pl.BlockSpec(memory_space=pltpu.VMEM)],
        out_specs=pl.BlockSpec(memory_space=pltpu.VMEM),
        scratch_shapes=[vmem(r) for r in rows1 + rows1 + rows2 + rows2]
        + [
            vmem(32 * sites),
            pltpu.SemaphoreType.DMA((6,)),
            pltpu.SemaphoreType.DMA((6,)),
        ],
        compiler_params=pltpu.CompilerParams(collective_id=0, has_side_effects=True),
        name="force",
    )(links.reshape(shape))
    return out.reshape(links.shape)


def solution(mesh):
    assert mesh.axis_names == ("gx", "gz", "ta")
    counts = tuple(mesh.shape[a] for a in AXES)
    spec = P(None, None, None, None, "ta", "gz", "gx")
    return jax.shard_map(
        functools.partial(per_device, counts),
        mesh=mesh,
        in_specs=(spec,),
        out_specs=spec,
        check_vma=False,
    )
```

```python
import functools

import jax
import jax.numpy as jnp
from jax import lax
from jax.experimental import pallas as pl
from jax.experimental.pallas import tpu as pltpu
from jax.sharding import PartitionSpec as P

NX = 16
COEFF = -1.9
AXES = ("ta", "gz", "gx")
SUB, LANES = 8, 128


def others(d):
    return [m for m in range(4) if m != d]


class Lattice:
    def __init__(self, depth):
        self.depth = depth
        self.per = SUB // depth
        self.ygroups = LANES // NX
        self.row = lax.broadcasted_iota(jnp.int32, (SUB, LANES), 0)
        self.lane = lax.broadcasted_iota(jnp.int32, (SUB, LANES), 1)
        self.zrow = self.row % depth
        self.xcol = self.lane % NX

    def rows(self, value, shift):
        shift %= SUB
        return pltpu.roll(value, shift, 0) if shift else value

    def lanes(self, value, shift):
        shift %= LANES
        return pltpu.roll(value, shift, 1) if shift else value


def entry(left, right, i, j, part, left_h, right_h):
    total = None
    for k in range(3):
        li = (k, i) if left_h else (i, k)
        ri = (j, k) if right_h else (k, j)
        lr, lm = left[0][li[0]][li[1]], left[1][li[0]][li[1]]
        rr, rm = right[0][ri[0]][ri[1]], right[1][ri[0]][ri[1]]
        if part == 0:
            first, second = lr * rr, lm * rm
            minus = left_h == right_h
        elif left_h:
            first, second = lr * rm, lm * rr
            minus = True
        else:
            first, second = lm * rr, lr * rm
            minus = right_h
        value = first - second if minus else first + second
        total = value if total is None else total + value
    return total


def product(left, right, left_h=False, right_h=False):
    return [
        [[entry(left, right, i, j, part, left_h, right_h) for j in range(3)] for i in range(3)]
        for part in range(2)
    ]


def projected(left, right, left_h=False, right_h=False):
    get = lambda i, j, part: entry(left, right, i, j, part, left_h, right_h)
    pairs = ((0, 1), (0, 2), (1, 2))
    real = [get(i, j, 0) - get(j, i, 0) for i, j in pairs]
    imag = [get(i, j, 1) + get(j, i, 1) for i, j in pairs]
    diag = [get(i, i, 1) for i in range(3)]
    third = (diag[0] + diag[1] + diag[2]) * (1.0 / 3.0)
    return real + imag + [diag[0] - third, diag[1] - third]


def third_row(real, imag):
    rows_r, rows_i = [], []
    for column in range(3):
        n, l = (column + 1) % 3, (column + 2) % 3
        rows_r.append(
            real[0][n] * real[1][l]
            - imag[0][n] * imag[1][l]
            - real[0][l] * real[1][n]
            + imag[0][l] * imag[1][n]
        )
        rows_i.append(
            real[0][l] * imag[1][n]
            + imag[0][l] * real[1][n]
            - real[0][n] * imag[1][l]
            - imag[0][n] * real[1][l]
        )
    return rows_r, rows_i


def sizes(depth, halves):
    yg = LANES // NX
    per = SUB // depth

    def rows(count):
        return (
            -(-count // per) * SUB,
            -(-count // depth) * SUB * halves,
            -(-count // yg) * SUB * halves,
        )

    return rows(36), rows(24)


PLANES = ((0, 3), (1, 3), (0, 2), (1, 2), (0, 1), (2, 3))


def force_terms(
    counts, depth, halves, hbm, acc,
    u, ahead_s, local_s, plaq_s, st, sz, sy, rt, rz, ry, qt, qz, qy, pt, pz, py,
    load_sem, send, recv,
):
    g = Lattice(depth)
    me = [lax.axis_index(a) for a in AXES]
    nxt = [lax.rem(me[i] + 1, counts[i]) for i in range(3)]
    prv = [lax.rem(me[i] + counts[i] - 1, counts[i]) for i in range(3)]

    def device(i, index):
        where = list(me)
        where[i] = index
        by = dict(zip(AXES, where))
        return (by["gx"], by["gz"], by["ta"])

    barrier = pltpu.get_barrier_semaphore()
    for i in range(3):
        for index in (nxt[i], prv[i]):
            pl.semaphore_signal(
                barrier, inc=1, device_id=device(i, index), device_id_type=pl.DeviceIdType.MESH
            )

    loads = {
        m: pltpu.make_async_copy(hbm.at[m, :, 0:2], u.at[m, :, 0:2], load_sem.at[m])
        for m in range(4)
    }
    last_rows = pltpu.make_async_copy(hbm.at[:, :, 2], u.at[:, :, 2], load_sem.at[4])
    for m in (3, 2, 1, 0):
        loads[m].start()
    last_rows.start()

    def load(m, part, i, j, h):
        return u[m, part, i, j, h * SUB : (h + 1) * SUB, :]

    def comps(d, m):
        return [(m, part, i, j) for part in range(2) for i in range(2) for j in range(3)]

    def all_comps(d):
        return [c for m in others(d) for c in comps(d, m)]

    def pack_t(m):
        cs, base = comps(0, m), 12 * others(0).index(m)
        for c0 in range(0, 12, g.per):
            value = None
            for k in range(g.per):
                x = g.rows(load(*cs[c0 + k], 0), depth * k)
                value = x if value is None else jnp.where(g.row >= depth * k, x, value)
            r = (base + c0) // g.per * SUB
            st[r : r + SUB, :] = value

    def pack_z(m):
        cs, base = comps(1, m), 12 * others(1).index(m)
        for c0 in range(0, 12, depth):
            for h in range(halves):
                value = None
                for k in range(depth):
                    x = g.rows(load(*cs[c0 + k], h), k)
                    value = x if value is None else jnp.where(g.zrow >= k, x, value)
                r = ((base + c0) // depth * halves + h) * SUB
                sz[r : r + SUB, :] = value

    def pack_y():
        cs = all_comps(2)
        for c0 in range(0, len(cs), g.ygroups):
            for h in range(halves):
                value = None
                for k in range(min(g.ygroups, len(cs) - c0)):
                    x = g.lanes(load(*cs[c0 + k], h), NX * k)
                    value = x if value is None else jnp.where(g.lane >= NX * k, x, value)
                r = (c0 // g.ygroups * halves + h) * SUB
                sy[r : r + SUB, :] = value

    for m in (3, 2, 1, 0):
        loads[m].wait()
        if m != 0:
            pack_t(m)
        if m != 1:
            pack_z(m)
    pack_y()

    def remote(src, dst, slot, i, index):
        return pltpu.make_async_remote_copy(
            src_ref=src, dst_ref=dst, send_sem=send.at[slot], recv_sem=recv.at[slot],
            device_id=device(i, index), device_id_type=pl.DeviceIdType.MESH,
        )

    def chunk(ref, d, m):
        n = ref.shape[0] // 3
        k = others(d).index(m)
        return ref.at[k * n : (k + 1) * n]

    first, second = {}, {}
    slot = 0
    for d, m in ((0, 3), (1, 3), (2, None), (0, 2), (1, 2), (0, 1), (1, 0)):
        src, dst = ((st, rt), (sz, rz), (sy, ry))[d]
        if m is not None:
            src, dst = chunk(src, d, m), chunk(dst, d, m)
        first[d, m] = remote(src, dst, slot, d, prv[d])
        slot += 1
    for d in range(3):
        src, dst = ((qt, pt), (qz, pz), (qy, py))[d]
        for m in others(d):
            second[d, m] = remote(chunk(src, d, m), chunk(dst, d, m), slot, d, nxt[d])
            slot += 1

    pl.semaphore_wait(barrier, 6)
    for copy in first.values():
        copy.start()
    last_rows.wait()

    def matrix(m, h):
        return [[[load(m, part, i, j, h) for j in range(3)] for i in range(3)] for part in range(2)]

    def save(ref, index, value):
        for part in range(2):
            for i in range(len(value[part])):
                for j in range(3):
                    ref[index, part, i, j] = value[part][i][j]

    def saved(ref, index, rows=3):
        return [[[ref[index, part, i, j] for j in range(3)] for i in range(rows)] for part in range(2)]

    def rolled(m, d, h, part, i, j):
        v = load(m, part, i, j, h)
        if d == 3:
            return jnp.where(g.xcol == NX - 1, g.lanes(v, NX - 1), g.lanes(v, -1))
        if d == 2:
            return g.lanes(v, -NX)
        if d == 1:
            return g.rows(v, -1)
        if h + 1 < halves:
            beyond = g.rows(load(m, part, i, j, h + 1), -depth)
            return jnp.where(g.row >= SUB - depth, beyond, g.rows(v, -depth))
        return g.rows(v, -depth)

    def complete(d, h):
        return d == 3 or (d == 0 and h + 1 < halves)

    slots = {}
    for mu, nu in PLANES:
        for h in range(halves):
            for m, d in ((nu, mu), (mu, nu)):
                slots[m, d, h] = len(slots)
                rows = 3 if complete(d, h) else 2
                save(
                    ahead_s, slots[m, d, h],
                    [[[rolled(m, d, h, part, i, j) for j in range(3)] for i in range(rows)] for part in range(2)],
                )
            save(
                local_s, PLANES.index((mu, nu)) * halves + h,
                product(matrix(mu, h), matrix(nu, h), left_h=True),
            )

    def ahead(m, d, h):
        if complete(d, h):
            return saved(ahead_s, slots[m, d, h])
        index = {c: n for n, c in enumerate(all_comps(d))}

        def get(part, i, j):
            v = ahead_s[slots[m, d, h], part, i, j]
            c = index[(m, part, i, j)]
            if d == 0:
                r = c // g.per * SUB
                edge = g.rows(rt[r : r + SUB, :], SUB - depth - depth * (c % g.per))
                return jnp.where(g.row >= SUB - depth, edge, v)
            if d == 1:
                r = (c // depth * halves + h) * SUB
                edge = g.rows(rz[r : r + SUB, :], depth - 1 - c % depth)
                return jnp.where(g.zrow == depth - 1, edge, v)
            r = (c // g.ygroups * halves + h) * SUB
            edge = g.lanes(ry[r : r + SUB, :], LANES - NX - NX * (c % g.ygroups))
            return jnp.where(g.lane >= LANES - NX, edge, v)

        real = [[get(0, i, j) for j in range(3)] for i in range(2)]
        imag = [[get(1, i, j) for j in range(3)] for i in range(2)]
        third_r, third_i = third_row(real, imag)
        return [real + [third_r], imag + [third_i]]

    seen = set()

    def add(m, c, h, value):
        r = ((m * 8 + c) * halves + h) * SUB
        if (m, c, h) in seen:
            acc[r : r + SUB, :] += value
        else:
            seen.add((m, c, h))
            acc[r : r + SUB, :] = value

    def lower(m, d, h, q):
        base = others(d).index(m) * 8
        if d == 2:
            for c0 in range(0, 8, g.ygroups):
                value = None
                for k in range(g.ygroups):
                    x = g.lanes(q[c0 + k], NX * (k + 1))
                    value = x if value is None else jnp.where(g.lane >= NX * k, x, value)
                r = ((base + c0) // g.ygroups * halves + h) * SUB
                qy[r : r + SUB, :] = value
        elif d == 1:
            for c0 in range(0, 8, depth):
                value = None
                for k in range(depth):
                    x = g.rows(q[c0 + k], k + 1 - depth)
                    value = x if value is None else jnp.where(g.zrow >= k, x, value)
                r = ((base + c0) // depth * halves + h) * SUB
                qz[r : r + SUB, :] = value
        elif d == 0 and h + 1 == halves:
            for c0 in range(0, 8, g.per):
                value = None
                for k in range(g.per):
                    x = g.rows(q[c0 + k], depth * (k + 1))
                    value = x if value is None else jnp.where(g.row >= depth * k, x, value)
                r = (base + c0) // g.per * SUB
                qt[r : r + SUB, :] = value
        for c in range(8):
            if d == 3:
                add(m, c, h, jnp.where(g.xcol == 0, g.lanes(q[c], 1 - NX), g.lanes(q[c], 1)))
            elif d == 2:
                add(m, c, h, jnp.where(g.lane >= NX, g.lanes(q[c], NX), 0.0))
            elif d == 1:
                add(m, c, h, jnp.where(g.zrow > 0, g.rows(q[c], 1), 0.0))
            else:
                moved = g.rows(q[c], depth)
                add(m, c, h, jnp.where(g.row >= depth, moved, 0.0))
                if h + 1 < halves:
                    add(m, c, h + 1, jnp.where(g.row < depth, moved, 0.0))

    waits = {(0, 3): [(0, 3)], (1, 3): [(1, 3)], (0, 2): [(0, 2), (2, None)], (1, 2): [(1, 2)], (0, 1): [(0, 1), (1, 0)]}
    for n, (mu, nu) in enumerate(PLANES):
        for h in range(halves):
            if h == (halves - 1 if (mu, nu) == (0, 3) else 0):
                for key in waits.get((mu, nu), ()):
                    first[key].wait_recv()
            a = product(ahead(nu, mu, h), ahead(mu, nu, h), right_h=True)
            save(plaq_s, n * halves + h, a)
            b = saved(local_s, n * halves + h)
            lower(mu, nu, h, projected(a, b, left_h=True))
            lower(nu, mu, h, projected(a, b, right_h=True))
        for key in ((mu, nu), (nu, mu)):
            if key in second:
                second[key].start()

    for n, (mu, nu) in enumerate(PLANES):
        for h in range(halves):
            e = product(matrix(mu, h), saved(plaq_s, n * halves + h))
            upper = projected(e, matrix(nu, h), right_h=True)
            for c in range(8):
                add(mu, c, h, upper[c])
                add(nu, c, h, -upper[c])

    for m in (2, 0, 1, 3):
        for d in others(m):
            if d < 3:
                second[d, m].wait_recv()
        for h in range(halves):
            for c in range(8):
                r = ((m * 8 + c) * halves + h) * SUB
                value = acc[r : r + SUB, :]
                for d in others(m):
                    b = others(d).index(m) * 8 + c
                    if d == 0 and h == 0:
                        s = b // g.per * SUB
                        x = g.rows(pt[s : s + SUB, :], -depth * (b % g.per))
                        value = value + jnp.where(g.row < depth, x, 0.0)
                    elif d == 1:
                        s = (b // depth * halves + h) * SUB
                        x = g.rows(pz[s : s + SUB, :], -(b % depth))
                        value = value + jnp.where(g.zrow == 0, x, 0.0)
                    elif d == 2:
                        s = (b // g.ygroups * halves + h) * SUB
                        x = g.lanes(py[s : s + SUB, :], -NX * (b % g.ygroups))
                        value = value + jnp.where(g.lane < NX, x, 0.0)
                acc[r : r + SUB, :] = value
    for copy in list(first.values()) + list(second.values()):
        copy.wait_send()


def expand(halves, acc, hbm, out, sems):
    copies = []
    for m in range(4):
        for h in range(halves):
            rows = [((m * 8 + c) * halves + h) * SUB for c in range(8)]
            f = [acc[r : r + SUB, :] * (COEFF * 0.5 if c < 6 else COEFF) for c, r in enumerate(rows)]

            def put(part, i, j, value):
                out[m, part, i, j, h * SUB : (h + 1) * SUB, :] = value

            for n, (i, j) in enumerate(((0, 1), (0, 2), (1, 2))):
                put(0, i, j, f[n])
                put(0, j, i, -f[n])
                put(1, i, j, f[3 + n])
                put(1, j, i, f[3 + n])
            for i in range(3):
                put(0, i, i, jnp.zeros((SUB, LANES), jnp.float32))
            put(1, 0, 0, f[6])
            put(1, 1, 1, f[7])
            put(1, 2, 2, -(f[6] + f[7]))
        copies.append(pltpu.make_async_copy(out.at[m], hbm.at[m], sems.at[m]))
        copies[-1].start()
    for copy in copies:
        copy.wait()


def per_device(counts, links):
    time_len, depth, flat = links.shape[4:]
    sites = time_len * depth
    assert flat == LANES and SUB % depth == 0 and sites % SUB == 0
    halves = sites // SUB
    rows1, rows2 = sizes(depth, halves)
    vmem = lambda *s: pltpu.VMEM(s + (LANES,), jnp.float32)
    shape = links.shape[:4] + (sites, flat)
    terms = pl.pallas_call(
        functools.partial(force_terms, counts, depth, halves),
        out_shape=pltpu.VMEM((32 * sites, flat), jnp.float32),
        in_specs=[pl.BlockSpec(memory_space=pl.ANY)],
        out_specs=pl.BlockSpec(memory_space=pltpu.VMEM),
        scratch_shapes=[
            vmem(*shape[:-1]),
            vmem(12 * halves, 2, 3, 3, SUB),
            vmem(6 * halves, 2, 3, 3, SUB),
            vmem(6 * halves, 2, 3, 3, SUB),
        ]
        + [vmem(r) for r in rows1 + rows1 + rows2 + rows2]
        + [
            pltpu.SemaphoreType.DMA((5,)),
            pltpu.SemaphoreType.DMA((16,)),
            pltpu.SemaphoreType.DMA((16,)),
        ],
        compiler_params=pltpu.CompilerParams(collective_id=0, has_side_effects=True),
        name="force_terms",
    )(links.reshape(shape))
    out = pl.pallas_call(
        functools.partial(expand, halves),
        out_shape=jax.ShapeDtypeStruct(shape, jnp.float32),
        in_specs=[pl.BlockSpec(memory_space=pltpu.VMEM)],
        out_specs=pl.BlockSpec(memory_space=pl.ANY),
        scratch_shapes=[vmem(*shape[:-1]), pltpu.SemaphoreType.DMA((4,))],
        name="expand",
    )(pltpu.with_memory_space_constraint(terms, pltpu.VMEM))
    return out.reshape(links.shape)


def solution(mesh):
    assert mesh.axis_names == ("gx", "gz", "ta")
    counts = tuple(mesh.shape[a] for a in AXES)
    spec = P(None, None, None, None, "ta", "gz", "gx")
    return jax.shard_map(
        functools.partial(per_device, counts),
        mesh=mesh,
        in_specs=(spec,),
        out_specs=spec,
        check_vma=False,
    )
```

```python
import functools

import jax
import jax.numpy as jnp
from jax import lax
from jax.experimental import pallas as pl
from jax.experimental.pallas import tpu as pltpu
from jax.sharding import PartitionSpec as P

NX = 16
COEFF = -1.9
AXES = ("ta", "gz", "gx")
SUB, LANES = 8, 128


def others(d):
    return [m for m in range(4) if m != d]


class Lattice:
    def __init__(self, depth):
        self.depth = depth
        self.per = SUB // depth
        self.ygroups = LANES // NX
        self.row = lax.broadcasted_iota(jnp.int32, (SUB, LANES), 0)
        self.lane = lax.broadcasted_iota(jnp.int32, (SUB, LANES), 1)
        self.zrow = self.row % depth
        self.xcol = self.lane % NX

    def rows(self, value, shift):
        shift %= SUB
        return pltpu.roll(value, shift, 0) if shift else value

    def lanes(self, value, shift):
        shift %= LANES
        return pltpu.roll(value, shift, 1) if shift else value


def entry(left, right, i, j, part, left_h, right_h):
    total = None
    for k in range(3):
        li = (k, i) if left_h else (i, k)
        ri = (j, k) if right_h else (k, j)
        lr, lm = left[0][li[0]][li[1]], left[1][li[0]][li[1]]
        rr, rm = right[0][ri[0]][ri[1]], right[1][ri[0]][ri[1]]
        if part == 0:
            first, second = lr * rr, lm * rm
            minus = left_h == right_h
        elif left_h:
            first, second = lr * rm, lm * rr
            minus = True
        else:
            first, second = lm * rr, lr * rm
            minus = right_h
        value = first - second if minus else first + second
        total = value if total is None else total + value
    return total


def product(left, right, left_h=False, right_h=False):
    return [
        [[entry(left, right, i, j, part, left_h, right_h) for j in range(3)] for i in range(3)]
        for part in range(2)
    ]


def projected(left, right, left_h=False, right_h=False):
    get = lambda i, j, part: entry(left, right, i, j, part, left_h, right_h)
    pairs = ((0, 1), (0, 2), (1, 2))
    real = [get(i, j, 0) - get(j, i, 0) for i, j in pairs]
    imag = [get(i, j, 1) + get(j, i, 1) for i, j in pairs]
    diag = [get(i, i, 1) for i in range(3)]
    third = (diag[0] + diag[1] + diag[2]) * (1.0 / 3.0)
    return real + imag + [diag[0] - third, diag[1] - third]


def third_row(real, imag):
    rows_r, rows_i = [], []
    for column in range(3):
        n, l = (column + 1) % 3, (column + 2) % 3
        rows_r.append(
            real[0][n] * real[1][l]
            - imag[0][n] * imag[1][l]
            - real[0][l] * real[1][n]
            + imag[0][l] * imag[1][n]
        )
        rows_i.append(
            real[0][l] * imag[1][n]
            + imag[0][l] * real[1][n]
            - real[0][n] * imag[1][l]
            - imag[0][n] * real[1][l]
        )
    return rows_r, rows_i


def sizes(depth, halves):
    yg = LANES // NX
    per = SUB // depth

    def rows(count):
        return (
            -(-count // per) * SUB,
            -(-count // depth) * SUB * halves,
            -(-count // yg) * SUB * halves,
        )

    return rows(36), rows(24)


PLANES = ((2, 3), (1, 3), (1, 2), (0, 3), (0, 2), (0, 1))


def force_terms(
    counts, depth, halves, hbm, acc,
    u, ahead_s, local_s, plaq_s, st, sz, sy, rt, rz, ry, qt, qz, qy, pt, pz, py,
    load_sem, send, recv,
):
    g = Lattice(depth)
    me = [lax.axis_index(a) for a in AXES]
    nxt = [lax.rem(me[i] + 1, counts[i]) for i in range(3)]
    prv = [lax.rem(me[i] + counts[i] - 1, counts[i]) for i in range(3)]

    def device(i, index):
        where = list(me)
        where[i] = index
        by = dict(zip(AXES, where))
        return (by["gx"], by["gz"], by["ta"])

    barrier = pltpu.get_barrier_semaphore()
    for i in range(3):
        for index in (nxt[i], prv[i]):
            pl.semaphore_signal(
                barrier, inc=1, device_id=device(i, index), device_id_type=pl.DeviceIdType.MESH
            )

    loads = {
        m: pltpu.make_async_copy(hbm.at[m, :, 0:2], u.at[m, :, 0:2], load_sem.at[m])
        for m in range(4)
    }
    last_rows = pltpu.make_async_copy(hbm.at[:, :, 2], u.at[:, :, 2], load_sem.at[4])
    for m in (3, 2, 1, 0):
        loads[m].start()
    last_rows.start()

    def load(m, part, i, j, h):
        return u[m, part, i, j, h * SUB : (h + 1) * SUB, :]

    def comps(d, m):
        return [(m, part, i, j) for part in range(2) for i in range(2) for j in range(3)]

    def all_comps(d):
        return [c for m in others(d) for c in comps(d, m)]

    def pack_t(m):
        cs, base = comps(0, m), 12 * others(0).index(m)
        for c0 in range(0, 12, g.per):
            value = None
            for k in range(g.per):
                x = g.rows(load(*cs[c0 + k], 0), depth * k)
                value = x if value is None else jnp.where(g.row >= depth * k, x, value)
            r = (base + c0) // g.per * SUB
            st[r : r + SUB, :] = value

    def pack_z(m):
        cs, base = comps(1, m), 12 * others(1).index(m)
        for c0 in range(0, 12, depth):
            for h in range(halves):
                value = None
                for k in range(depth):
                    x = g.rows(load(*cs[c0 + k], h), k)
                    value = x if value is None else jnp.where(g.zrow >= k, x, value)
                r = ((base + c0) // depth * halves + h) * SUB
                sz[r : r + SUB, :] = value

    def pack_y():
        cs = all_comps(2)
        for c0 in range(0, len(cs), g.ygroups):
            for h in range(halves):
                value = None
                for k in range(min(g.ygroups, len(cs) - c0)):
                    x = g.lanes(load(*cs[c0 + k], h), NX * k)
                    value = x if value is None else jnp.where(g.lane >= NX * k, x, value)
                r = (c0 // g.ygroups * halves + h) * SUB
                sy[r : r + SUB, :] = value

    for m in (3, 2, 1, 0):
        loads[m].wait()
        if m != 0:
            pack_t(m)
        if m != 1:
            pack_z(m)
    pack_y()

    def remote(src, dst, slot, i, index):
        return pltpu.make_async_remote_copy(
            src_ref=src, dst_ref=dst, send_sem=send.at[slot], recv_sem=recv.at[slot],
            device_id=device(i, index), device_id_type=pl.DeviceIdType.MESH,
        )

    def chunk(ref, d, m):
        n = ref.shape[0] // 3
        k = others(d).index(m)
        return ref.at[k * n : (k + 1) * n]

    first, second = {}, {}
    slot = 0
    for d, m in ((0, 3), (0, 2), (0, 1), (1, 3), (1, 2), (1, 0), (2, None)):
        src, dst = ((st, rt), (sz, rz), (sy, ry))[d]
        if m is not None:
            src, dst = chunk(src, d, m), chunk(dst, d, m)
        first[d, m] = remote(src, dst, slot, d, prv[d])
        slot += 1
    for d in range(3):
        src, dst = ((qt, pt), (qz, pz), (qy, py))[d]
        for m in others(d):
            second[d, m] = remote(chunk(src, d, m), chunk(dst, d, m), slot, d, nxt[d])
            slot += 1

    pl.semaphore_wait(barrier, 6)
    for copy in first.values():
        copy.start()
    last_rows.wait()

    def matrix(m, h):
        return [[[load(m, part, i, j, h) for j in range(3)] for i in range(3)] for part in range(2)]

    def save(ref, index, value):
        for part in range(2):
            for i in range(len(value[part])):
                for j in range(3):
                    ref[index, part, i, j] = value[part][i][j]

    def saved(ref, index, rows=3):
        return [[[ref[index, part, i, j] for j in range(3)] for i in range(rows)] for part in range(2)]

    def rolled(m, d, h, part, i, j):
        v = load(m, part, i, j, h)
        if d == 3:
            return jnp.where(g.xcol == NX - 1, g.lanes(v, NX - 1), g.lanes(v, -1))
        if d == 2:
            return g.lanes(v, -NX)
        if d == 1:
            return g.rows(v, -1)
        if h + 1 < halves:
            beyond = g.rows(load(m, part, i, j, h + 1), -depth)
            return jnp.where(g.row >= SUB - depth, beyond, g.rows(v, -depth))
        return g.rows(v, -depth)

    def complete(d, h):
        return d == 3 or (d == 0 and h + 1 < halves)

    slots = {}
    for mu, nu in PLANES:
        for h in range(halves):
            for m, d in ((nu, mu), (mu, nu)):
                slots[m, d, h] = len(slots)
                rows = 3 if complete(d, h) else 2
                save(
                    ahead_s, slots[m, d, h],
                    [[[rolled(m, d, h, part, i, j) for j in range(3)] for i in range(rows)] for part in range(2)],
                )
            save(
                local_s, PLANES.index((mu, nu)) * halves + h,
                product(matrix(mu, h), matrix(nu, h), left_h=True),
            )

    def ahead(m, d, h):
        if complete(d, h):
            return saved(ahead_s, slots[m, d, h])
        index = {c: n for n, c in enumerate(all_comps(d))}

        def get(part, i, j):
            v = ahead_s[slots[m, d, h], part, i, j]
            c = index[(m, part, i, j)]
            if d == 0:
                r = c // g.per * SUB
                edge = g.rows(rt[r : r + SUB, :], SUB - depth - depth * (c % g.per))
                return jnp.where(g.row >= SUB - depth, edge, v)
            if d == 1:
                r = (c // depth * halves + h) * SUB
                edge = g.rows(rz[r : r + SUB, :], depth - 1 - c % depth)
                return jnp.where(g.zrow == depth - 1, edge, v)
            r = (c // g.ygroups * halves + h) * SUB
            edge = g.lanes(ry[r : r + SUB, :], LANES - NX - NX * (c % g.ygroups))
            return jnp.where(g.lane >= LANES - NX, edge, v)

        real = [[get(0, i, j) for j in range(3)] for i in range(2)]
        imag = [[get(1, i, j) for j in range(3)] for i in range(2)]
        third_r, third_i = third_row(real, imag)
        return [real + [third_r], imag + [third_i]]

    seen = set()

    def add(m, c, h, value):
        r = ((m * 8 + c) * halves + h) * SUB
        if (m, c, h) in seen:
            acc[r : r + SUB, :] += value
        else:
            seen.add((m, c, h))
            acc[r : r + SUB, :] = value

    def lower(m, d, h, q):
        base = others(d).index(m) * 8
        if d == 2:
            for c0 in range(0, 8, g.ygroups):
                value = None
                for k in range(g.ygroups):
                    x = g.lanes(q[c0 + k], NX * (k + 1))
                    value = x if value is None else jnp.where(g.lane >= NX * k, x, value)
                r = ((base + c0) // g.ygroups * halves + h) * SUB
                qy[r : r + SUB, :] = value
        elif d == 1:
            for c0 in range(0, 8, depth):
                value = None
                for k in range(depth):
                    x = g.rows(q[c0 + k], k + 1 - depth)
                    value = x if value is None else jnp.where(g.zrow >= k, x, value)
                r = ((base + c0) // depth * halves + h) * SUB
                qz[r : r + SUB, :] = value
        elif d == 0 and h + 1 == halves:
            for c0 in range(0, 8, g.per):
                value = None
                for k in range(g.per):
                    x = g.rows(q[c0 + k], depth * (k + 1))
                    value = x if value is None else jnp.where(g.row >= depth * k, x, value)
                r = (base + c0) // g.per * SUB
                qt[r : r + SUB, :] = value
        for c in range(8):
            if d == 3:
                add(m, c, h, jnp.where(g.xcol == 0, g.lanes(q[c], 1 - NX), g.lanes(q[c], 1)))
            elif d == 2:
                add(m, c, h, jnp.where(g.lane >= NX, g.lanes(q[c], NX), 0.0))
            elif d == 1:
                add(m, c, h, jnp.where(g.zrow > 0, g.rows(q[c], 1), 0.0))
            else:
                moved = g.rows(q[c], depth)
                add(m, c, h, jnp.where(g.row >= depth, moved, 0.0))
                if h + 1 < halves:
                    add(m, c, h + 1, jnp.where(g.row < depth, moved, 0.0))

    steps = [(pair, h) for pair in PLANES if pair[0] for h in range(halves)]
    steps += [(pair, h) for h in range(halves) for pair in PLANES if not pair[0]]
    arrived, left = set(), {key: halves for key in second}
    for (mu, nu), h in steps:
        n = PLANES.index((mu, nu))
        for d, m in ((mu, nu), (nu, mu)):
            key = (d, None if d == 2 else m)
            if key in first and key not in arrived and not complete(d, h):
                arrived.add(key)
                first[key].wait_recv()
        a = product(ahead(nu, mu, h), ahead(mu, nu, h), right_h=True)
        save(plaq_s, n * halves + h, a)
        b = saved(local_s, n * halves + h)
        lower(mu, nu, h, projected(a, b, left_h=True))
        lower(nu, mu, h, projected(a, b, right_h=True))
        for key in ((mu, nu), (nu, mu)):
            if key in second:
                left[key] -= 1
                if not left[key]:
                    second[key].start()

    for n, (mu, nu) in enumerate(PLANES):
        for h in range(halves):
            e = product(matrix(mu, h), saved(plaq_s, n * halves + h))
            upper = projected(e, matrix(nu, h), right_h=True)
            for c in range(8):
                add(mu, c, h, upper[c])
                add(nu, c, h, -upper[c])

    for m in (3, 2, 1, 0):
        for d in others(m):
            if d in (1, 2):
                second[d, m].wait_recv()
        for h in range(halves):
            for c in range(8):
                r = ((m * 8 + c) * halves + h) * SUB
                value = acc[r : r + SUB, :]
                for d in others(m):
                    b = others(d).index(m) * 8 + c
                    if d == 1:
                        s = (b // depth * halves + h) * SUB
                        x = g.rows(pz[s : s + SUB, :], -(b % depth))
                        value = value + jnp.where(g.zrow == 0, x, 0.0)
                    elif d == 2:
                        s = (b // g.ygroups * halves + h) * SUB
                        x = g.lanes(py[s : s + SUB, :], -NX * (b % g.ygroups))
                        value = value + jnp.where(g.lane < NX, x, 0.0)
                acc[r : r + SUB, :] = value
    for m in (3, 2, 1):
        second[0, m].wait_recv()
        for c in range(8):
            r = (m * 8 + c) * halves * SUB
            b = others(0).index(m) * 8 + c
            s = b // g.per * SUB
            x = g.rows(pt[s : s + SUB, :], -depth * (b % g.per))
            acc[r : r + SUB, :] += jnp.where(g.row < depth, x, 0.0)
    for copy in list(first.values()) + list(second.values()):
        copy.wait_send()


def expand(halves, acc, hbm, out, sems):
    copies = []
    for m in range(4):
        for h in range(halves):
            rows = [((m * 8 + c) * halves + h) * SUB for c in range(8)]
            f = [acc[r : r + SUB, :] * (COEFF * 0.5 if c < 6 else COEFF) for c, r in enumerate(rows)]

            def put(part, i, j, value):
                out[m, part, i, j, h * SUB : (h + 1) * SUB, :] = value

            for n, (i, j) in enumerate(((0, 1), (0, 2), (1, 2))):
                put(0, i, j, f[n])
                put(0, j, i, -f[n])
                put(1, i, j, f[3 + n])
                put(1, j, i, f[3 + n])
            for i in range(3):
                put(0, i, i, jnp.zeros((SUB, LANES), jnp.float32))
            put(1, 0, 0, f[6])
            put(1, 1, 1, f[7])
            put(1, 2, 2, -(f[6] + f[7]))
        copies.append(pltpu.make_async_copy(out.at[m], hbm.at[m], sems.at[m]))
        copies[-1].start()
    for copy in copies:
        copy.wait()


def per_device(counts, links):
    time_len, depth, flat = links.shape[4:]
    sites = time_len * depth
    assert flat == LANES and SUB % depth == 0 and sites % SUB == 0
    halves = sites // SUB
    rows1, rows2 = sizes(depth, halves)
    vmem = lambda *s: pltpu.VMEM(s + (LANES,), jnp.float32)
    shape = links.shape[:4] + (sites, flat)
    terms = pl.pallas_call(
        functools.partial(force_terms, counts, depth, halves),
        out_shape=pltpu.VMEM((32 * sites, flat), jnp.float32),
        in_specs=[pl.BlockSpec(memory_space=pl.ANY)],
        out_specs=pl.BlockSpec(memory_space=pltpu.VMEM),
        scratch_shapes=[
            vmem(*shape[:-1]),
            vmem(12 * halves, 2, 3, 3, SUB),
            vmem(6 * halves, 2, 3, 3, SUB),
            vmem(6 * halves, 2, 3, 3, SUB),
        ]
        + [vmem(r) for r in rows1 + rows1 + rows2 + rows2]
        + [
            pltpu.SemaphoreType.DMA((5,)),
            pltpu.SemaphoreType.DMA((16,)),
            pltpu.SemaphoreType.DMA((16,)),
        ],
        compiler_params=pltpu.CompilerParams(collective_id=0, has_side_effects=True),
        name="force_terms",
    )(links.reshape(shape))
    out = pl.pallas_call(
        functools.partial(expand, halves),
        out_shape=jax.ShapeDtypeStruct(shape, jnp.float32),
        in_specs=[pl.BlockSpec(memory_space=pltpu.VMEM)],
        out_specs=pl.BlockSpec(memory_space=pl.ANY),
        scratch_shapes=[vmem(*shape[:-1]), pltpu.SemaphoreType.DMA((4,))],
        name="expand",
    )(pltpu.with_memory_space_constraint(terms, pltpu.VMEM))
    return out.reshape(links.shape)


def solution(mesh):
    assert mesh.axis_names == ("gx", "gz", "ta")
    counts = tuple(mesh.shape[a] for a in AXES)
    spec = P(None, None, None, None, "ta", "gz", "gx")
    return jax.shard_map(
        functools.partial(per_device, counts),
        mesh=mesh,
        in_specs=(spec,),
        out_specs=spec,
        check_vma=False,
    )
```

```python
import functools

import jax
import jax.numpy as jnp
from jax import lax
from jax.experimental import pallas as pl
from jax.experimental.pallas import tpu as pltpu
from jax.sharding import PartitionSpec as P

NX = 16
COEFF = -1.9
AXES = ("ta", "gz", "gx")
SUB, LANES = 8, 128


def others(d):
    return [m for m in range(4) if m != d]


class Lattice:
    def __init__(self, depth):
        self.depth = depth
        self.per = SUB // depth
        self.ygroups = LANES // NX
        self.row = lax.broadcasted_iota(jnp.int32, (SUB, LANES), 0)
        self.lane = lax.broadcasted_iota(jnp.int32, (SUB, LANES), 1)
        self.zrow = self.row % depth
        self.xcol = self.lane % NX

    def rows(self, value, shift):
        shift %= SUB
        return pltpu.roll(value, shift, 0) if shift else value

    def lanes(self, value, shift):
        shift %= LANES
        return pltpu.roll(value, shift, 1) if shift else value


def entry(left, right, i, j, part, left_h, right_h):
    total = None
    for k in range(3):
        li = (k, i) if left_h else (i, k)
        ri = (j, k) if right_h else (k, j)
        lr, lm = left[0][li[0]][li[1]], left[1][li[0]][li[1]]
        rr, rm = right[0][ri[0]][ri[1]], right[1][ri[0]][ri[1]]
        if part == 0:
            first, second = lr * rr, lm * rm
            minus = left_h == right_h
        elif left_h:
            first, second = lr * rm, lm * rr
            minus = True
        else:
            first, second = lm * rr, lr * rm
            minus = right_h
        value = first - second if minus else first + second
        total = value if total is None else total + value
    return total


def product(left, right, left_h=False, right_h=False):
    return [
        [[entry(left, right, i, j, part, left_h, right_h) for j in range(3)] for i in range(3)]
        for part in range(2)
    ]


def projected(left, right, left_h=False, right_h=False):
    get = lambda i, j, part: entry(left, right, i, j, part, left_h, right_h)
    pairs = ((0, 1), (0, 2), (1, 2))
    real = [get(i, j, 0) - get(j, i, 0) for i, j in pairs]
    imag = [get(i, j, 1) + get(j, i, 1) for i, j in pairs]
    diag = [get(i, i, 1) for i in range(3)]
    third = (diag[0] + diag[1] + diag[2]) * (1.0 / 3.0)
    return real + imag + [diag[0] - third, diag[1] - third]


def third_row(real, imag):
    rows_r, rows_i = [], []
    for column in range(3):
        n, l = (column + 1) % 3, (column + 2) % 3
        rows_r.append(
            real[0][n] * real[1][l]
            - imag[0][n] * imag[1][l]
            - real[0][l] * real[1][n]
            + imag[0][l] * imag[1][n]
        )
        rows_i.append(
            real[0][l] * imag[1][n]
            + imag[0][l] * real[1][n]
            - real[0][n] * imag[1][l]
            - imag[0][n] * real[1][l]
        )
    return rows_r, rows_i


def sizes(depth, halves):
    yg = LANES // NX
    per = SUB // depth

    def rows(count):
        return (
            -(-count // per) * SUB,
            -(-count // depth) * SUB * halves,
            -(-count // yg) * SUB * halves,
        )

    return rows(36), rows(24)


PLANES = ((2, 3), (1, 3), (1, 2), (0, 3), (0, 2), (0, 1))


def force_terms(
    counts, depth, halves, hbm, acc,
    u, ahead_s, local_s, plaq_s, st, sz, sy, rt, rz, ry, qz, qy, pz, py, bs, br, ezs, ezr, eys, eyr,
    load_sem, send, recv,
):
    g = Lattice(depth)
    me = [lax.axis_index(a) for a in AXES]
    nxt = [lax.rem(me[i] + 1, counts[i]) for i in range(3)]
    prv = [lax.rem(me[i] + counts[i] - 1, counts[i]) for i in range(3)]

    def device(i, index):
        where = list(me)
        where[i] = index
        by = dict(zip(AXES, where))
        return (by["gx"], by["gz"], by["ta"])

    def diagonal(time, i, index):
        where = list(me)
        where[0], where[i] = time, index
        by = dict(zip(AXES, where))
        return (by["gx"], by["gz"], by["ta"])

    barrier = pltpu.get_barrier_semaphore()
    for i in (1, 2):
        for where in (diagonal(nxt[0], i, prv[i]), diagonal(prv[0], i, nxt[i])):
            pl.semaphore_signal(
                barrier, inc=1, device_id=where, device_id_type=pl.DeviceIdType.MESH
            )
    for i in range(3):
        for index in (nxt[i], prv[i]):
            pl.semaphore_signal(
                barrier, inc=1, device_id=device(i, index), device_id_type=pl.DeviceIdType.MESH
            )

    loads = {
        m: pltpu.make_async_copy(hbm.at[m, :, 0:2], u.at[m, :, 0:2], load_sem.at[m])
        for m in range(4)
    }
    last_rows = pltpu.make_async_copy(hbm.at[:, :, 2], u.at[:, :, 2], load_sem.at[4])
    for m in (3, 2, 1, 0):
        loads[m].start()
    last_rows.start()

    def load(m, part, i, j, h):
        return u[m, part, i, j, h * SUB : (h + 1) * SUB, :]

    def comps(d, m):
        return [(m, part, i, j) for part in range(2) for i in range(2) for j in range(3)]

    def all_comps(d):
        return [c for m in others(d) for c in comps(d, m)]

    def pack_t(m):
        cs, base = comps(0, m), 12 * others(0).index(m)
        for c0 in range(0, 12, g.per):
            value = None
            for k in range(g.per):
                x = g.rows(load(*cs[c0 + k], 0), depth * k)
                value = x if value is None else jnp.where(g.row >= depth * k, x, value)
            r = (base + c0) // g.per * SUB
            st[r : r + SUB, :] = value

    def pack_z(m):
        cs, base = comps(1, m), 12 * others(1).index(m)
        for c0 in range(0, 12, depth):
            for h in range(halves):
                value = None
                for k in range(depth):
                    x = g.rows(load(*cs[c0 + k], h), k)
                    value = x if value is None else jnp.where(g.zrow >= k, x, value)
                r = ((base + c0) // depth * halves + h) * SUB
                sz[r : r + SUB, :] = value

    def pack_y():
        cs = all_comps(2)
        for c0 in range(0, len(cs), g.ygroups):
            for h in range(halves):
                value = None
                for k in range(min(g.ygroups, len(cs) - c0)):
                    x = g.lanes(load(*cs[c0 + k], h), NX * k)
                    value = x if value is None else jnp.where(g.lane >= NX * k, x, value)
                r = (c0 // g.ygroups * halves + h) * SUB
                sy[r : r + SUB, :] = value

    def pack_back(m):
        cs = comps(0, m)
        for c0 in range(0, 12, g.per):
            value = None
            for k in range(g.per):
                x = g.rows(load(*cs[c0 + k], halves - 1), depth * (k + 1))
                value = x if value is None else jnp.where(g.row >= depth * k, x, value)
            r = (12 * m + c0) // g.per * SUB
            bs[r : r + SUB, :] = value

    def pack_edges():
        cs = comps(0, 0)
        for c0 in range(0, 12, SUB):
            rows = lanes = None
            for k in range(min(SUB, 12 - c0)):
                v = load(*cs[c0 + k], halves - 1)
                x = g.rows(v, k - (SUB - depth))
                rows = x if rows is None else jnp.where(g.row >= k, x, rows)
            ezs[c0 : c0 + SUB, :] = rows
        for c0 in range(0, 12, g.ygroups):
            for k in range(min(g.ygroups, 12 - c0)):
                x = g.lanes(g.rows(load(*cs[c0 + k], halves - 1), depth), NX * k)
                lanes = x if k == 0 else jnp.where(g.lane >= NX * k, x, lanes)
            r = c0 // g.ygroups * SUB
            eys[r : r + SUB, :] = lanes

    for m in (3, 2, 1, 0):
        loads[m].wait()
        pack_back(m)
        if m != 0:
            pack_t(m)
        if m != 1:
            pack_z(m)
    pack_y()
    pack_edges()

    def remote(src, dst, slot, i, index):
        return pltpu.make_async_remote_copy(
            src_ref=src, dst_ref=dst, send_sem=send.at[slot], recv_sem=recv.at[slot],
            device_id=device(i, index), device_id_type=pl.DeviceIdType.MESH,
        )

    def chunk(ref, d, m):
        n = ref.shape[0] // 3
        k = others(d).index(m)
        return ref.at[k * n : (k + 1) * n]

    first, second = {}, {}
    slot = 0
    for d, m in ((0, 3), (0, 2), (0, 1), (1, 3), (1, 2), (1, 0), (2, None)):
        src, dst = ((st, rt), (sz, rz), (sy, ry))[d]
        if m is not None:
            src, dst = chunk(src, d, m), chunk(dst, d, m)
        first[d, m] = remote(src, dst, slot, d, prv[d])
        slot += 1
    back = {}
    for m in range(4):
        n = bs.shape[0] // 4
        back[m] = remote(bs.at[m * n : (m + 1) * n], br.at[m * n : (m + 1) * n], slot, 0, nxt[0])
        slot += 1
    for i, src, dst in ((1, ezs, ezr), (2, eys, eyr)):
        back["edge", i] = pltpu.make_async_remote_copy(
            src_ref=src, dst_ref=dst, send_sem=send.at[slot], recv_sem=recv.at[slot],
            device_id=diagonal(nxt[0], i, prv[i]), device_id_type=pl.DeviceIdType.MESH,
        )
        slot += 1
    for d in (1, 2):
        src, dst = (None, (qz, pz), (qy, py))[d]
        for m in others(d):
            second[d, m] = remote(chunk(src, d, m), chunk(dst, d, m), slot, d, nxt[d])
            slot += 1

    pl.semaphore_wait(barrier, 10)
    for copy in list(first.values()) + [back[k] for k in (("edge", 1), ("edge", 2), 0, 3, 2, 1)]:
        copy.start()
    last_rows.wait()

    def matrix(m, h):
        return [[[load(m, part, i, j, h) for j in range(3)] for i in range(3)] for part in range(2)]

    def save(ref, index, value):
        for part in range(2):
            for i in range(len(value[part])):
                for j in range(3):
                    ref[index, part, i, j] = value[part][i][j]

    def saved(ref, index, rows=3):
        return [[[ref[index, part, i, j] for j in range(3)] for i in range(rows)] for part in range(2)]

    def rolled(m, d, h, part, i, j):
        v = load(m, part, i, j, h)
        if d == 3:
            return jnp.where(g.xcol == NX - 1, g.lanes(v, NX - 1), g.lanes(v, -1))
        if d == 2:
            return g.lanes(v, -NX)
        if d == 1:
            return g.rows(v, -1)
        if h + 1 < halves:
            beyond = g.rows(load(m, part, i, j, h + 1), -depth)
            return jnp.where(g.row >= SUB - depth, beyond, g.rows(v, -depth))
        return g.rows(v, -depth)

    def complete(d, h):
        return d == 3 or (d == 0 and h + 1 < halves)

    slots = {}
    for mu, nu in PLANES:
        for h in range(halves):
            for m, d in ((nu, mu), (mu, nu)):
                slots[m, d, h] = len(slots)
                rows = 3 if complete(d, h) else 2
                save(
                    ahead_s, slots[m, d, h],
                    [[[rolled(m, d, h, part, i, j) for j in range(3)] for i in range(rows)] for part in range(2)],
                )
            save(
                local_s, PLANES.index((mu, nu)) * halves + h,
                product(matrix(mu, h), matrix(nu, h), left_h=True),
            )

    def ahead(m, d, h):
        if complete(d, h):
            return saved(ahead_s, slots[m, d, h])
        index = {c: n for n, c in enumerate(all_comps(d))}

        def get(part, i, j):
            v = ahead_s[slots[m, d, h], part, i, j]
            c = index[(m, part, i, j)]
            if d == 0:
                r = c // g.per * SUB
                edge = g.rows(rt[r : r + SUB, :], SUB - depth - depth * (c % g.per))
                return jnp.where(g.row >= SUB - depth, edge, v)
            if d == 1:
                r = (c // depth * halves + h) * SUB
                edge = g.rows(rz[r : r + SUB, :], depth - 1 - c % depth)
                return jnp.where(g.zrow == depth - 1, edge, v)
            r = (c // g.ygroups * halves + h) * SUB
            edge = g.lanes(ry[r : r + SUB, :], LANES - NX - NX * (c % g.ygroups))
            return jnp.where(g.lane >= LANES - NX, edge, v)

        real = [[get(0, i, j) for j in range(3)] for i in range(2)]
        imag = [[get(1, i, j) for j in range(3)] for i in range(2)]
        third_r, third_i = third_row(real, imag)
        return [real + [third_r], imag + [third_i]]

    seen = set()

    def add(m, c, h, value):
        r = ((m * 8 + c) * halves + h) * SUB
        if (m, c, h) in seen:
            acc[r : r + SUB, :] += value
        else:
            seen.add((m, c, h))
            acc[r : r + SUB, :] = value

    def lower(m, d, h, q):
        base = others(d).index(m) * 8
        if d == 2:
            for c0 in range(0, 8, g.ygroups):
                value = None
                for k in range(g.ygroups):
                    x = g.lanes(q[c0 + k], NX * (k + 1))
                    value = x if value is None else jnp.where(g.lane >= NX * k, x, value)
                r = ((base + c0) // g.ygroups * halves + h) * SUB
                qy[r : r + SUB, :] = value
        elif d == 1:
            for c0 in range(0, 8, depth):
                value = None
                for k in range(depth):
                    x = g.rows(q[c0 + k], k + 1 - depth)
                    value = x if value is None else jnp.where(g.zrow >= k, x, value)
                r = ((base + c0) // depth * halves + h) * SUB
                qz[r : r + SUB, :] = value
        for c in range(8):
            if d == 3:
                add(m, c, h, jnp.where(g.xcol == 0, g.lanes(q[c], 1 - NX), g.lanes(q[c], 1)))
            elif d == 2:
                add(m, c, h, jnp.where(g.lane >= NX, g.lanes(q[c], NX), 0.0))
            elif d == 1:
                add(m, c, h, jnp.where(g.zrow > 0, g.rows(q[c], 1), 0.0))
            else:
                moved = g.rows(q[c], depth)
                add(m, c, h, jnp.where(g.row >= depth, moved, 0.0))
                if h + 1 < halves:
                    add(m, c, h + 1, jnp.where(g.row < depth, moved, 0.0))

    steps = [(pair, h) for pair in PLANES if pair[0] for h in range(halves)]
    steps += [(pair, h) for h in range(halves) for pair in PLANES if not pair[0]]
    arrived, left = set(), {key: halves for key in second}
    for (mu, nu), h in steps:
        n = PLANES.index((mu, nu))
        for d, m in ((mu, nu), (nu, mu)):
            key = (d, None if d == 2 else m)
            if key in first and key not in arrived and not complete(d, h):
                arrived.add(key)
                first[key].wait_recv()
        a = product(ahead(nu, mu, h), ahead(mu, nu, h), right_h=True)
        save(plaq_s, n * halves + h, a)
        b = saved(local_s, n * halves + h)
        lower(mu, nu, h, projected(a, b, left_h=True))
        lower(nu, mu, h, projected(a, b, right_h=True))
        for key in ((mu, nu), (nu, mu)):
            if key in second:
                left[key] -= 1
                if not left[key]:
                    second[key].start()

    for n, (mu, nu) in enumerate(PLANES):
        for h in range(halves):
            e = product(matrix(mu, h), saved(plaq_s, n * halves + h))
            upper = projected(e, matrix(nu, h), right_h=True)
            for c in range(8):
                add(mu, c, h, upper[c])
                add(nu, c, h, -upper[c])

    def complete_rows(get):
        real = [[get(0, i, j) for j in range(3)] for i in range(2)]
        imag = [[get(1, i, j) for j in range(3)] for i in range(2)]
        third_r, third_i = third_row(real, imag)
        return [real + [third_r], imag + [third_i]]

    def behind(m):
        def get(part, i, j):
            c = 12 * m + part * 6 + i * 3 + j
            r = c // g.per * SUB
            return g.rows(br[r : r + SUB, :], -depth * (c % g.per))

        return complete_rows(get)

    for key in (("edge", 1), ("edge", 2), 0):
        back[key].wait_recv()
    time_link = behind(0)
    for m in (3, 2, 1):
        back[m].wait_recv()

        def step(part, i, j):
            v = time_link[part][i][j]
            c = part * 6 + i * 3 + j
            if m == 3:
                return jnp.where(g.xcol == NX - 1, g.lanes(v, NX - 1), g.lanes(v, -1))
            if m == 1:
                r = c // SUB * SUB
                edge = g.rows(ezr[r : r + SUB, :], depth - 1 - c % SUB)
                return jnp.where(g.row == depth - 1, edge, g.rows(v, -1))
            r = c // g.ygroups * SUB
            edge = g.lanes(eyr[r : r + SUB, :], LANES - NX - NX * (c % g.ygroups))
            return jnp.where(g.lane >= LANES - NX, edge, g.lanes(v, -NX))

        a = product(matrix(m, 0), complete_rows(step), right_h=True)
        b = product(time_link, behind(m), left_h=True)
        q = projected(a, b, right_h=True)
        for c in range(8):
            add(m, c, 0, jnp.where(g.row < depth, q[c], 0.0))

    for m in (3, 2, 1, 0):
        for d in others(m):
            if d in (1, 2):
                second[d, m].wait_recv()
        for h in range(halves):
            for c in range(8):
                r = ((m * 8 + c) * halves + h) * SUB
                value = acc[r : r + SUB, :]
                for d in others(m):
                    b = others(d).index(m) * 8 + c
                    if d == 1:
                        s = (b // depth * halves + h) * SUB
                        x = g.rows(pz[s : s + SUB, :], -(b % depth))
                        value = value + jnp.where(g.zrow == 0, x, 0.0)
                    elif d == 2:
                        s = (b // g.ygroups * halves + h) * SUB
                        x = g.lanes(py[s : s + SUB, :], -NX * (b % g.ygroups))
                        value = value + jnp.where(g.lane < NX, x, 0.0)
                acc[r : r + SUB, :] = value
    for copy in list(first.values()) + list(back.values()) + list(second.values()):
        copy.wait_send()


def expand(halves, acc, hbm, out, sems):
    copies = []
    for m in range(4):
        for h in range(halves):
            rows = [((m * 8 + c) * halves + h) * SUB for c in range(8)]
            f = [acc[r : r + SUB, :] * (COEFF * 0.5 if c < 6 else COEFF) for c, r in enumerate(rows)]

            def put(part, i, j, value):
                out[m, part, i, j, h * SUB : (h + 1) * SUB, :] = value

            for n, (i, j) in enumerate(((0, 1), (0, 2), (1, 2))):
                put(0, i, j, f[n])
                put(0, j, i, -f[n])
                put(1, i, j, f[3 + n])
                put(1, j, i, f[3 + n])
            for i in range(3):
                put(0, i, i, jnp.zeros((SUB, LANES), jnp.float32))
            put(1, 0, 0, f[6])
            put(1, 1, 1, f[7])
            put(1, 2, 2, -(f[6] + f[7]))
        copies.append(pltpu.make_async_copy(out.at[m], hbm.at[m], sems.at[m]))
        copies[-1].start()
    for copy in copies:
        copy.wait()


def per_device(counts, links):
    time_len, depth, flat = links.shape[4:]
    sites = time_len * depth
    assert flat == LANES and SUB % depth == 0 and sites % SUB == 0
    halves = sites // SUB
    rows1, rows2 = sizes(depth, halves)
    vmem = lambda *s: pltpu.VMEM(s + (LANES,), jnp.float32)
    shape = links.shape[:4] + (sites, flat)
    terms = pl.pallas_call(
        functools.partial(force_terms, counts, depth, halves),
        out_shape=pltpu.VMEM((32 * sites, flat), jnp.float32),
        in_specs=[pl.BlockSpec(memory_space=pl.ANY)],
        out_specs=pl.BlockSpec(memory_space=pltpu.VMEM),
        scratch_shapes=[
            vmem(*shape[:-1]),
            vmem(12 * halves, 2, 3, 3, SUB),
            vmem(6 * halves, 2, 3, 3, SUB),
            vmem(6 * halves, 2, 3, 3, SUB),
        ]
        + [vmem(r) for r in rows1 + rows1 + rows2[1:] + rows2[1:]]
        + [vmem(r) for r in (rows1[0] // 3 * 4,) * 2 + (2 * SUB,) * 4]
        + [
            pltpu.SemaphoreType.DMA((5,)),
            pltpu.SemaphoreType.DMA((19,)),
            pltpu.SemaphoreType.DMA((19,)),
        ],
        compiler_params=pltpu.CompilerParams(collective_id=0, has_side_effects=True),
        name="force_terms",
    )(links.reshape(shape))
    out = pl.pallas_call(
        functools.partial(expand, halves),
        out_shape=jax.ShapeDtypeStruct(shape, jnp.float32),
        in_specs=[pl.BlockSpec(memory_space=pltpu.VMEM)],
        out_specs=pl.BlockSpec(memory_space=pl.ANY),
        scratch_shapes=[vmem(*shape[:-1]), pltpu.SemaphoreType.DMA((4,))],
        name="expand",
    )(pltpu.with_memory_space_constraint(terms, pltpu.VMEM))
    return out.reshape(links.shape)


def solution(mesh):
    assert mesh.axis_names == ("gx", "gz", "ta")
    counts = tuple(mesh.shape[a] for a in AXES)
    spec = P(None, None, None, None, "ta", "gz", "gx")
    return jax.shard_map(
        functools.partial(per_device, counts),
        mesh=mesh,
        in_specs=(spec,),
        out_specs=spec,
        check_vma=False,
    )
```

```python
import functools

import jax
import jax.numpy as jnp
from jax import lax
from jax.experimental import pallas as pl
from jax.experimental.pallas import tpu as pltpu
from jax.sharding import PartitionSpec as P

NX = 16
COEFF = -1.9
AXES = ("ta", "gz", "gx")
SUB, LANES = 8, 128


def others(d):
    return [m for m in range(4) if m != d]


class Lattice:
    def __init__(self, depth):
        self.depth = depth
        self.per = SUB // depth
        self.ygroups = LANES // NX
        self.row = lax.broadcasted_iota(jnp.int32, (SUB, LANES), 0)
        self.lane = lax.broadcasted_iota(jnp.int32, (SUB, LANES), 1)
        self.zrow = self.row % depth
        self.xcol = self.lane % NX

    def rows(self, value, shift):
        shift %= SUB
        return pltpu.roll(value, shift, 0) if shift else value

    def lanes(self, value, shift):
        shift %= LANES
        return pltpu.roll(value, shift, 1) if shift else value


def entry(left, right, i, j, part, left_h, right_h):
    total = None
    for k in range(3):
        li = (k, i) if left_h else (i, k)
        ri = (j, k) if right_h else (k, j)
        lr, lm = left[0][li[0]][li[1]], left[1][li[0]][li[1]]
        rr, rm = right[0][ri[0]][ri[1]], right[1][ri[0]][ri[1]]
        if part == 0:
            first, second = lr * rr, lm * rm
            minus = left_h == right_h
        elif left_h:
            first, second = lr * rm, lm * rr
            minus = True
        else:
            first, second = lm * rr, lr * rm
            minus = right_h
        value = first - second if minus else first + second
        total = value if total is None else total + value
    return total


def product(left, right, left_h=False, right_h=False):
    return [
        [[entry(left, right, i, j, part, left_h, right_h) for j in range(3)] for i in range(3)]
        for part in range(2)
    ]


def projected(left, right, left_h=False, right_h=False):
    get = lambda i, j, part: entry(left, right, i, j, part, left_h, right_h)
    pairs = ((0, 1), (0, 2), (1, 2))
    real = [get(i, j, 0) - get(j, i, 0) for i, j in pairs]
    imag = [get(i, j, 1) + get(j, i, 1) for i, j in pairs]
    diag = [get(i, i, 1) for i in range(3)]
    third = (diag[0] + diag[1] + diag[2]) * (1.0 / 3.0)
    return real + imag + [diag[0] - third, diag[1] - third]


def third_row(real, imag):
    rows_r, rows_i = [], []
    for column in range(3):
        n, l = (column + 1) % 3, (column + 2) % 3
        rows_r.append(
            real[0][n] * real[1][l]
            - imag[0][n] * imag[1][l]
            - real[0][l] * real[1][n]
            + imag[0][l] * imag[1][n]
        )
        rows_i.append(
            real[0][l] * imag[1][n]
            + imag[0][l] * real[1][n]
            - real[0][n] * imag[1][l]
            - imag[0][n] * real[1][l]
        )
    return rows_r, rows_i


def sizes(depth, halves):
    yg = LANES // NX
    per = SUB // depth

    def rows(count):
        return (
            -(-count // per) * SUB,
            -(-count // depth) * SUB * halves,
            -(-count // yg) * SUB * halves,
        )

    return rows(36), rows(24)


PLANES = ((2, 3), (1, 3), (1, 2), (0, 1), (0, 2), (0, 3))


def force_terms(
    counts, depth, halves, hbm, acc,
    u, ahead_s, local_s, plaq_s, st, sz, sy, rt, rz, ry, qz, qy, pz, py, bs, br, ezs, ezr, eys, eyr,
    load_sem, send, recv,
):
    g = Lattice(depth)
    me = [lax.axis_index(a) for a in AXES]
    nxt = [lax.rem(me[i] + 1, counts[i]) for i in range(3)]
    prv = [lax.rem(me[i] + counts[i] - 1, counts[i]) for i in range(3)]

    def device(i, index):
        where = list(me)
        where[i] = index
        by = dict(zip(AXES, where))
        return (by["gx"], by["gz"], by["ta"])

    def diagonal(time, i, index):
        where = list(me)
        where[0], where[i] = time, index
        by = dict(zip(AXES, where))
        return (by["gx"], by["gz"], by["ta"])

    barrier = pltpu.get_barrier_semaphore()
    for i in (1, 2):
        for where in (diagonal(nxt[0], i, prv[i]), diagonal(prv[0], i, nxt[i])):
            pl.semaphore_signal(
                barrier, inc=1, device_id=where, device_id_type=pl.DeviceIdType.MESH
            )
    for i in range(3):
        for index in (nxt[i], prv[i]):
            pl.semaphore_signal(
                barrier, inc=1, device_id=device(i, index), device_id_type=pl.DeviceIdType.MESH
            )

    loads = {
        m: pltpu.make_async_copy(hbm.at[m, :, 0:2], u.at[m, :, 0:2], load_sem.at[m])
        for m in range(4)
    }
    last_rows = pltpu.make_async_copy(hbm.at[:, :, 2], u.at[:, :, 2], load_sem.at[4])
    for m in (3, 2, 1, 0):
        loads[m].start()
    last_rows.start()

    def load(m, part, i, j, h):
        return u[m, part, i, j, h * SUB : (h + 1) * SUB, :]

    def comps(d, m):
        return [(m, part, i, j) for part in range(2) for i in range(2) for j in range(3)]

    def all_comps(d):
        return [c for m in others(d) for c in comps(d, m)]

    def pack_t(m):
        cs, base = comps(0, m), 12 * others(0).index(m)
        for c0 in range(0, 12, g.per):
            value = None
            for k in range(g.per):
                x = g.rows(load(*cs[c0 + k], 0), depth * k)
                value = x if value is None else jnp.where(g.row >= depth * k, x, value)
            r = (base + c0) // g.per * SUB
            st[r : r + SUB, :] = value

    def pack_z(m):
        cs, base = comps(1, m), 12 * others(1).index(m)
        for c0 in range(0, 12, depth):
            for h in range(halves):
                value = None
                for k in range(depth):
                    x = g.rows(load(*cs[c0 + k], h), k)
                    value = x if value is None else jnp.where(g.zrow >= k, x, value)
                r = ((base + c0) // depth * halves + h) * SUB
                sz[r : r + SUB, :] = value

    def pack_y():
        cs = all_comps(2)
        for c0 in range(0, len(cs), g.ygroups):
            for h in range(halves):
                value = None
                for k in range(min(g.ygroups, len(cs) - c0)):
                    x = g.lanes(load(*cs[c0 + k], h), NX * k)
                    value = x if value is None else jnp.where(g.lane >= NX * k, x, value)
                r = (c0 // g.ygroups * halves + h) * SUB
                sy[r : r + SUB, :] = value

    def pack_back(m):
        cs = comps(0, m)
        for c0 in range(0, 12, g.per):
            value = None
            for k in range(g.per):
                x = g.rows(load(*cs[c0 + k], halves - 1), depth * (k + 1))
                value = x if value is None else jnp.where(g.row >= depth * k, x, value)
            r = (12 * m + c0) // g.per * SUB
            bs[r : r + SUB, :] = value

    def pack_edges():
        cs = comps(0, 0)
        for c0 in range(0, 12, SUB):
            rows = lanes = None
            for k in range(min(SUB, 12 - c0)):
                v = load(*cs[c0 + k], halves - 1)
                x = g.rows(v, k - (SUB - depth))
                rows = x if rows is None else jnp.where(g.row >= k, x, rows)
            ezs[c0 : c0 + SUB, :] = rows
        for c0 in range(0, 12, g.ygroups):
            for k in range(min(g.ygroups, 12 - c0)):
                x = g.lanes(g.rows(load(*cs[c0 + k], halves - 1), depth), NX * k)
                lanes = x if k == 0 else jnp.where(g.lane >= NX * k, x, lanes)
            r = c0 // g.ygroups * SUB
            eys[r : r + SUB, :] = lanes

    for m in (3, 2, 1, 0):
        loads[m].wait()
        pack_back(m)
        if m != 0:
            pack_t(m)
        if m != 1:
            pack_z(m)
    pack_y()
    pack_edges()

    def remote(src, dst, slot, i, index):
        return pltpu.make_async_remote_copy(
            src_ref=src, dst_ref=dst, send_sem=send.at[slot], recv_sem=recv.at[slot],
            device_id=device(i, index), device_id_type=pl.DeviceIdType.MESH,
        )

    def chunk(ref, d, m):
        n = ref.shape[0] // 3
        k = others(d).index(m)
        return ref.at[k * n : (k + 1) * n]

    first, second = {}, {}
    slot = 0
    for d, m in ((0, 1), (0, 2), (0, 3), (1, 3), (1, 2), (1, 0), (2, None)):
        src, dst = ((st, rt), (sz, rz), (sy, ry))[d]
        if m is not None:
            src, dst = chunk(src, d, m), chunk(dst, d, m)
        first[d, m] = remote(src, dst, slot, d, prv[d])
        slot += 1
    back = {}
    for m in range(4):
        n = bs.shape[0] // 4
        back[m] = remote(bs.at[m * n : (m + 1) * n], br.at[m * n : (m + 1) * n], slot, 0, nxt[0])
        slot += 1
    for i, src, dst in ((1, ezs, ezr), (2, eys, eyr)):
        back["edge", i] = pltpu.make_async_remote_copy(
            src_ref=src, dst_ref=dst, send_sem=send.at[slot], recv_sem=recv.at[slot],
            device_id=diagonal(nxt[0], i, prv[i]), device_id_type=pl.DeviceIdType.MESH,
        )
        slot += 1
    for d in (1, 2):
        src, dst = (None, (qz, pz), (qy, py))[d]
        for m in others(d):
            second[d, m] = remote(chunk(src, d, m), chunk(dst, d, m), slot, d, nxt[d])
            slot += 1

    pl.semaphore_wait(barrier, 10)
    for key, copy in first.items():
        if key[0]:
            copy.start()
    low_faces = [copy for key, copy in first.items() if not key[0]]
    high_faces = [back[key] for key in (("edge", 1), ("edge", 2), 0, 3, 2, 1)]
    around = me[0] == counts[0] - 1

    @pl.when(around)
    def _():
        for copy in high_faces + low_faces:
            copy.start()

    @pl.when(jnp.logical_not(around))
    def _():
        for copy in low_faces + high_faces:
            copy.start()

    last_rows.wait()

    def matrix(m, h):
        return [[[load(m, part, i, j, h) for j in range(3)] for i in range(3)] for part in range(2)]

    def save(ref, index, value):
        for part in range(2):
            for i in range(len(value[part])):
                for j in range(3):
                    ref[index, part, i, j] = value[part][i][j]

    def saved(ref, index, rows=3):
        return [[[ref[index, part, i, j] for j in range(3)] for i in range(rows)] for part in range(2)]

    def rolled(m, d, h, part, i, j):
        v = load(m, part, i, j, h)
        if d == 3:
            return jnp.where(g.xcol == NX - 1, g.lanes(v, NX - 1), g.lanes(v, -1))
        if d == 2:
            return g.lanes(v, -NX)
        if d == 1:
            return g.rows(v, -1)
        if h + 1 < halves:
            beyond = g.rows(load(m, part, i, j, h + 1), -depth)
            return jnp.where(g.row >= SUB - depth, beyond, g.rows(v, -depth))
        return g.rows(v, -depth)

    def complete(d, h):
        return d == 3 or (d == 0 and h + 1 < halves)

    slots = {}
    for mu, nu in PLANES:
        for h in range(halves):
            for m, d in ((nu, mu), (mu, nu)):
                slots[m, d, h] = len(slots)
                rows = 3 if complete(d, h) else 2
                save(
                    ahead_s, slots[m, d, h],
                    [[[rolled(m, d, h, part, i, j) for j in range(3)] for i in range(rows)] for part in range(2)],
                )
            save(
                local_s, PLANES.index((mu, nu)) * halves + h,
                product(matrix(mu, h), matrix(nu, h), left_h=True),
            )

    def ahead(m, d, h):
        if complete(d, h):
            return saved(ahead_s, slots[m, d, h])
        index = {c: n for n, c in enumerate(all_comps(d))}

        def get(part, i, j):
            v = ahead_s[slots[m, d, h], part, i, j]
            c = index[(m, part, i, j)]
            if d == 0:
                r = c // g.per * SUB
                edge = g.rows(rt[r : r + SUB, :], SUB - depth - depth * (c % g.per))
                return jnp.where(g.row >= SUB - depth, edge, v)
            if d == 1:
                r = (c // depth * halves + h) * SUB
                edge = g.rows(rz[r : r + SUB, :], depth - 1 - c % depth)
                return jnp.where(g.zrow == depth - 1, edge, v)
            r = (c // g.ygroups * halves + h) * SUB
            edge = g.lanes(ry[r : r + SUB, :], LANES - NX - NX * (c % g.ygroups))
            return jnp.where(g.lane >= LANES - NX, edge, v)

        real = [[get(0, i, j) for j in range(3)] for i in range(2)]
        imag = [[get(1, i, j) for j in range(3)] for i in range(2)]
        third_r, third_i = third_row(real, imag)
        return [real + [third_r], imag + [third_i]]

    seen = set()

    def add(m, c, h, value):
        r = ((m * 8 + c) * halves + h) * SUB
        if (m, c, h) in seen:
            acc[r : r + SUB, :] += value
        else:
            seen.add((m, c, h))
            acc[r : r + SUB, :] = value

    def lower(m, d, h, q):
        base = others(d).index(m) * 8
        if d == 2:
            for c0 in range(0, 8, g.ygroups):
                value = None
                for k in range(g.ygroups):
                    x = g.lanes(q[c0 + k], NX * (k + 1))
                    value = x if value is None else jnp.where(g.lane >= NX * k, x, value)
                r = ((base + c0) // g.ygroups * halves + h) * SUB
                qy[r : r + SUB, :] = value
        elif d == 1:
            for c0 in range(0, 8, depth):
                value = None
                for k in range(depth):
                    x = g.rows(q[c0 + k], k + 1 - depth)
                    value = x if value is None else jnp.where(g.zrow >= k, x, value)
                r = ((base + c0) // depth * halves + h) * SUB
                qz[r : r + SUB, :] = value
        for c in range(8):
            if d == 3:
                add(m, c, h, jnp.where(g.xcol == 0, g.lanes(q[c], 1 - NX), g.lanes(q[c], 1)))
            elif d == 2:
                add(m, c, h, jnp.where(g.lane >= NX, g.lanes(q[c], NX), 0.0))
            elif d == 1:
                add(m, c, h, jnp.where(g.zrow > 0, g.rows(q[c], 1), 0.0))
            else:
                moved = g.rows(q[c], depth)
                add(m, c, h, jnp.where(g.row >= depth, moved, 0.0))
                if h + 1 < halves:
                    add(m, c, h + 1, jnp.where(g.row < depth, moved, 0.0))

    steps = [(pair, h) for pair in PLANES if pair[0] for h in range(halves)]
    steps += [(pair, h) for h in range(halves) for pair in PLANES if not pair[0]]
    arrived, left = set(), {key: halves for key in second}
    for (mu, nu), h in steps:
        n = PLANES.index((mu, nu))
        for d, m in ((mu, nu), (nu, mu)):
            key = (d, None if d == 2 else m)
            if key in first and key not in arrived and not complete(d, h):
                arrived.add(key)
                first[key].wait_recv()
        a = product(ahead(nu, mu, h), ahead(mu, nu, h), right_h=True)
        save(plaq_s, n * halves + h, a)
        b = saved(local_s, n * halves + h)
        lower(mu, nu, h, projected(a, b, left_h=True))
        lower(nu, mu, h, projected(a, b, right_h=True))
        for key in ((mu, nu), (nu, mu)):
            if key in second:
                left[key] -= 1
                if not left[key]:
                    second[key].start()

    for n, (mu, nu) in enumerate(PLANES):
        for h in range(halves):
            e = product(matrix(mu, h), saved(plaq_s, n * halves + h))
            upper = projected(e, matrix(nu, h), right_h=True)
            for c in range(8):
                add(mu, c, h, upper[c])
                add(nu, c, h, -upper[c])

    def complete_rows(get):
        real = [[get(0, i, j) for j in range(3)] for i in range(2)]
        imag = [[get(1, i, j) for j in range(3)] for i in range(2)]
        third_r, third_i = third_row(real, imag)
        return [real + [third_r], imag + [third_i]]

    def behind(m):
        def get(part, i, j):
            c = 12 * m + part * 6 + i * 3 + j
            r = c // g.per * SUB
            return g.rows(br[r : r + SUB, :], -depth * (c % g.per))

        return complete_rows(get)

    for key in (("edge", 1), ("edge", 2), 0):
        back[key].wait_recv()
    time_link = behind(0)
    for m in (3, 2, 1):
        back[m].wait_recv()

        def step(part, i, j):
            v = time_link[part][i][j]
            c = part * 6 + i * 3 + j
            if m == 3:
                return jnp.where(g.xcol == NX - 1, g.lanes(v, NX - 1), g.lanes(v, -1))
            if m == 1:
                r = c // SUB * SUB
                edge = g.rows(ezr[r : r + SUB, :], depth - 1 - c % SUB)
                return jnp.where(g.row == depth - 1, edge, g.rows(v, -1))
            r = c // g.ygroups * SUB
            edge = g.lanes(eyr[r : r + SUB, :], LANES - NX - NX * (c % g.ygroups))
            return jnp.where(g.lane >= LANES - NX, edge, g.lanes(v, -NX))

        a = product(matrix(m, 0), complete_rows(step), right_h=True)
        b = product(time_link, behind(m), left_h=True)
        q = projected(a, b, right_h=True)
        for c in range(8):
            add(m, c, 0, jnp.where(g.row < depth, q[c], 0.0))

    for m in (3, 2, 1, 0):
        for d in others(m):
            if d in (1, 2):
                second[d, m].wait_recv()
        for h in range(halves):
            for c in range(8):
                r = ((m * 8 + c) * halves + h) * SUB
                value = acc[r : r + SUB, :]
                for d in others(m):
                    b = others(d).index(m) * 8 + c
                    if d == 1:
                        s = (b // depth * halves + h) * SUB
                        x = g.rows(pz[s : s + SUB, :], -(b % depth))
                        value = value + jnp.where(g.zrow == 0, x, 0.0)
                    elif d == 2:
                        s = (b // g.ygroups * halves + h) * SUB
                        x = g.lanes(py[s : s + SUB, :], -NX * (b % g.ygroups))
                        value = value + jnp.where(g.lane < NX, x, 0.0)
                acc[r : r + SUB, :] = value
    for copy in list(first.values()) + list(back.values()) + list(second.values()):
        copy.wait_send()


def expand(halves, acc, hbm, out, sems):
    copies = []
    for m in range(4):
        for h in range(halves):
            rows = [((m * 8 + c) * halves + h) * SUB for c in range(8)]
            f = [acc[r : r + SUB, :] * (COEFF * 0.5 if c < 6 else COEFF) for c, r in enumerate(rows)]

            def put(part, i, j, value):
                out[m, part, i, j, h * SUB : (h + 1) * SUB, :] = value

            for n, (i, j) in enumerate(((0, 1), (0, 2), (1, 2))):
                put(0, i, j, f[n])
                put(0, j, i, -f[n])
                put(1, i, j, f[3 + n])
                put(1, j, i, f[3 + n])
            for i in range(3):
                put(0, i, i, jnp.zeros((SUB, LANES), jnp.float32))
            put(1, 0, 0, f[6])
            put(1, 1, 1, f[7])
            put(1, 2, 2, -(f[6] + f[7]))
        copies.append(pltpu.make_async_copy(out.at[m], hbm.at[m], sems.at[m]))
        copies[-1].start()
    for copy in copies:
        copy.wait()


def per_device(counts, links):
    time_len, depth, flat = links.shape[4:]
    sites = time_len * depth
    assert flat == LANES and SUB % depth == 0 and sites % SUB == 0
    halves = sites // SUB
    rows1, rows2 = sizes(depth, halves)
    vmem = lambda *s: pltpu.VMEM(s + (LANES,), jnp.float32)
    shape = links.shape[:4] + (sites, flat)
    terms = pl.pallas_call(
        functools.partial(force_terms, counts, depth, halves),
        out_shape=pltpu.VMEM((32 * sites, flat), jnp.float32),
        in_specs=[pl.BlockSpec(memory_space=pl.ANY)],
        out_specs=pl.BlockSpec(memory_space=pltpu.VMEM),
        scratch_shapes=[
            vmem(*shape[:-1]),
            vmem(12 * halves, 2, 3, 3, SUB),
            vmem(6 * halves, 2, 3, 3, SUB),
            vmem(6 * halves, 2, 3, 3, SUB),
        ]
        + [vmem(r) for r in rows1 + rows1 + rows2[1:] + rows2[1:]]
        + [vmem(r) for r in (rows1[0] // 3 * 4,) * 2 + (2 * SUB,) * 4]
        + [
            pltpu.SemaphoreType.DMA((5,)),
            pltpu.SemaphoreType.DMA((19,)),
            pltpu.SemaphoreType.DMA((19,)),
        ],
        compiler_params=pltpu.CompilerParams(collective_id=0, has_side_effects=True),
        name="force_terms",
    )(links.reshape(shape))
    out = pl.pallas_call(
        functools.partial(expand, halves),
        out_shape=jax.ShapeDtypeStruct(shape, jnp.float32),
        in_specs=[pl.BlockSpec(memory_space=pltpu.VMEM)],
        out_specs=pl.BlockSpec(memory_space=pl.ANY),
        scratch_shapes=[vmem(*shape[:-1]), pltpu.SemaphoreType.DMA((4,))],
        name="expand",
    )(pltpu.with_memory_space_constraint(terms, pltpu.VMEM))
    return out.reshape(links.shape)


def solution(mesh):
    assert mesh.axis_names == ("gx", "gz", "ta")
    counts = tuple(mesh.shape[a] for a in AXES)
    spec = P(None, None, None, None, "ta", "gz", "gx")
    return jax.shard_map(
        functools.partial(per_device, counts),
        mesh=mesh,
        in_specs=(spec,),
        out_specs=spec,
        check_vma=False,
    )
```

```python
import functools

import jax
import jax.numpy as jnp
from jax import lax
from jax.experimental import pallas as pl
from jax.experimental.pallas import tpu as pltpu
from jax.sharding import PartitionSpec as P

NX = 16
COEFF = -1.9
AXES = ("ta", "gz", "gx")
SUB, LANES = 8, 128


def others(d):
    return [m for m in range(4) if m != d]


class Lattice:
    def __init__(self, depth):
        self.depth = depth
        self.per = SUB // depth
        self.ygroups = LANES // NX
        self.row = lax.broadcasted_iota(jnp.int32, (SUB, LANES), 0)
        self.lane = lax.broadcasted_iota(jnp.int32, (SUB, LANES), 1)
        self.zrow = self.row % depth
        self.xcol = self.lane % NX

    def rows(self, value, shift):
        shift %= SUB
        return pltpu.roll(value, shift, 0) if shift else value

    def lanes(self, value, shift):
        shift %= LANES
        return pltpu.roll(value, shift, 1) if shift else value


def entry(left, right, i, j, part, left_h, right_h):
    total = None
    for k in range(3):
        li = (k, i) if left_h else (i, k)
        ri = (j, k) if right_h else (k, j)
        lr, lm = left[0][li[0]][li[1]], left[1][li[0]][li[1]]
        rr, rm = right[0][ri[0]][ri[1]], right[1][ri[0]][ri[1]]
        if part == 0:
            first, second = lr * rr, lm * rm
            minus = left_h == right_h
        elif left_h:
            first, second = lr * rm, lm * rr
            minus = True
        else:
            first, second = lm * rr, lr * rm
            minus = right_h
        value = first - second if minus else first + second
        total = value if total is None else total + value
    return total


def product(left, right, left_h=False, right_h=False):
    return [
        [[entry(left, right, i, j, part, left_h, right_h) for j in range(3)] for i in range(3)]
        for part in range(2)
    ]


def projected(left, right, left_h=False, right_h=False):
    get = lambda i, j, part: entry(left, right, i, j, part, left_h, right_h)
    pairs = ((0, 1), (0, 2), (1, 2))
    real = [get(i, j, 0) - get(j, i, 0) for i, j in pairs]
    imag = [get(i, j, 1) + get(j, i, 1) for i, j in pairs]
    diag = [get(i, i, 1) for i in range(3)]
    third = (diag[0] + diag[1] + diag[2]) * (1.0 / 3.0)
    return real + imag + [diag[0] - third, diag[1] - third]


def third_row(real, imag):
    rows_r, rows_i = [], []
    for column in range(3):
        n, l = (column + 1) % 3, (column + 2) % 3
        rows_r.append(
            real[0][n] * real[1][l]
            - imag[0][n] * imag[1][l]
            - real[0][l] * real[1][n]
            + imag[0][l] * imag[1][n]
        )
        rows_i.append(
            real[0][l] * imag[1][n]
            + imag[0][l] * real[1][n]
            - real[0][n] * imag[1][l]
            - imag[0][n] * real[1][l]
        )
    return rows_r, rows_i


def sizes(depth, halves):
    yg = LANES // NX
    per = SUB // depth

    def rows(count):
        return (
            -(-count // per) * SUB,
            -(-count // depth) * SUB * halves,
            -(-count // yg) * SUB * halves,
        )

    return rows(36), rows(24)


PLANES = ((2, 3), (1, 3), (1, 2), (0, 1), (0, 2), (0, 3))


def force_terms(
    counts, depth, halves, hbm, acc,
    u, ahead_s, local_s, plaq_s, st, sz, sy, rt, rz, ry, qz, qy, pz, py, bs, br, ezs, ezr, eys, eyr,
    load_sem, send, recv,
):
    g = Lattice(depth)
    me = [lax.axis_index(a) for a in AXES]
    nxt = [lax.rem(me[i] + 1, counts[i]) for i in range(3)]
    prv = [lax.rem(me[i] + counts[i] - 1, counts[i]) for i in range(3)]

    def device(i, index):
        where = list(me)
        where[i] = index
        by = dict(zip(AXES, where))
        return (by["gx"], by["gz"], by["ta"])

    def diagonal(time, i, index):
        where = list(me)
        where[0], where[i] = time, index
        by = dict(zip(AXES, where))
        return (by["gx"], by["gz"], by["ta"])

    barrier = pltpu.get_barrier_semaphore()
    for i in (1, 2):
        for where in (diagonal(nxt[0], i, prv[i]), diagonal(prv[0], i, nxt[i])):
            pl.semaphore_signal(
                barrier, inc=1, device_id=where, device_id_type=pl.DeviceIdType.MESH
            )
    for i in range(3):
        for index in (nxt[i], prv[i]):
            pl.semaphore_signal(
                barrier, inc=1, device_id=device(i, index), device_id_type=pl.DeviceIdType.MESH
            )

    loads = {
        m: pltpu.make_async_copy(hbm.at[m, :, 0:2], u.at[m, :, 0:2], load_sem.at[m])
        for m in range(4)
    }
    last_rows = pltpu.make_async_copy(hbm.at[:, :, 2], u.at[:, :, 2], load_sem.at[4])
    for m in (3, 2, 1, 0):
        loads[m].start()
    last_rows.start()

    def load(m, part, i, j, h):
        return u[m, part, i, j, h * SUB : (h + 1) * SUB, :]

    def comps(d, m):
        return [(m, part, i, j) for part in range(2) for i in range(2) for j in range(3)]

    def all_comps(d):
        return [c for m in others(d) for c in comps(d, m)]

    def pack_t(m):
        cs, base = comps(0, m), 12 * others(0).index(m)
        for c0 in range(0, 12, g.per):
            value = None
            for k in range(g.per):
                x = g.rows(load(*cs[c0 + k], 0), depth * k)
                value = x if value is None else jnp.where(g.row >= depth * k, x, value)
            r = (base + c0) // g.per * SUB
            st[r : r + SUB, :] = value

    def pack_z(m):
        cs, base = comps(1, m), 12 * others(1).index(m)
        for c0 in range(0, 12, depth):
            for h in range(halves):
                value = None
                for k in range(depth):
                    x = g.rows(load(*cs[c0 + k], h), k)
                    value = x if value is None else jnp.where(g.zrow >= k, x, value)
                r = ((base + c0) // depth * halves + h) * SUB
                sz[r : r + SUB, :] = value

    def pack_y():
        cs = all_comps(2)
        for c0 in range(0, len(cs), g.ygroups):
            for h in range(halves):
                value = None
                for k in range(min(g.ygroups, len(cs) - c0)):
                    x = g.lanes(load(*cs[c0 + k], h), NX * k)
                    value = x if value is None else jnp.where(g.lane >= NX * k, x, value)
                r = (c0 // g.ygroups * halves + h) * SUB
                sy[r : r + SUB, :] = value

    def pack_back(m):
        cs = comps(0, m)
        for c0 in range(0, 12, g.per):
            value = None
            for k in range(g.per):
                x = g.rows(load(*cs[c0 + k], halves - 1), depth * (k + 1))
                value = x if value is None else jnp.where(g.row >= depth * k, x, value)
            r = (12 * m + c0) // g.per * SUB
            bs[r : r + SUB, :] = value

    def pack_edges():
        cs = comps(0, 0)
        for c0 in range(0, 12, SUB):
            rows = lanes = None
            for k in range(min(SUB, 12 - c0)):
                v = load(*cs[c0 + k], halves - 1)
                x = g.rows(v, k - (SUB - depth))
                rows = x if rows is None else jnp.where(g.row >= k, x, rows)
            ezs[c0 : c0 + SUB, :] = rows
        for c0 in range(0, 12, g.ygroups):
            for k in range(min(g.ygroups, 12 - c0)):
                x = g.lanes(g.rows(load(*cs[c0 + k], halves - 1), depth), NX * k)
                lanes = x if k == 0 else jnp.where(g.lane >= NX * k, x, lanes)
            r = c0 // g.ygroups * SUB
            eys[r : r + SUB, :] = lanes

    for m in (3, 2, 1, 0):
        loads[m].wait()
        pack_back(m)
        if m != 0:
            pack_t(m)
        if m != 1:
            pack_z(m)
    pack_y()
    pack_edges()

    def remote(src, dst, slot, i, index):
        return pltpu.make_async_remote_copy(
            src_ref=src, dst_ref=dst, send_sem=send.at[slot], recv_sem=recv.at[slot],
            device_id=device(i, index), device_id_type=pl.DeviceIdType.MESH,
        )

    def chunk(ref, d, m):
        n = ref.shape[0] // 3
        k = others(d).index(m)
        return ref.at[k * n : (k + 1) * n]

    first, second = {}, {}
    slot = 0
    for d, m in ((0, 1), (0, 2), (0, 3), (1, 3), (1, 2), (1, 0), (2, None)):
        src, dst = ((st, rt), (sz, rz), (sy, ry))[d]
        if m is not None:
            src, dst = chunk(src, d, m), chunk(dst, d, m)
        first[d, m] = remote(src, dst, slot, d, prv[d])
        slot += 1
    back = {}
    for m in range(4):
        n = bs.shape[0] // 4
        back[m] = remote(bs.at[m * n : (m + 1) * n], br.at[m * n : (m + 1) * n], slot, 0, nxt[0])
        slot += 1
    for i, src, dst in ((1, ezs, ezr), (2, eys, eyr)):
        back["edge", i] = pltpu.make_async_remote_copy(
            src_ref=src, dst_ref=dst, send_sem=send.at[slot], recv_sem=recv.at[slot],
            device_id=diagonal(nxt[0], i, prv[i]), device_id_type=pl.DeviceIdType.MESH,
        )
        slot += 1
    for d in (1, 2):
        src, dst = (None, (qz, pz), (qy, py))[d]
        for m in others(d):
            second[d, m] = remote(chunk(src, d, m), chunk(dst, d, m), slot, d, nxt[d])
            slot += 1

    pl.semaphore_wait(barrier, 10)
    for key, copy in first.items():
        if key[0]:
            copy.start()
    low_faces = [copy for key, copy in first.items() if not key[0]]
    high_faces = [back[key] for key in (("edge", 1), ("edge", 2), 0, 3, 2, 1)]
    around = me[0] == counts[0] - 1

    @pl.when(around)
    def _():
        for copy in high_faces + low_faces:
            copy.start()

    @pl.when(jnp.logical_not(around))
    def _():
        for copy in low_faces + high_faces:
            copy.start()

    last_rows.wait()

    def matrix(m, h):
        return [[[load(m, part, i, j, h) for j in range(3)] for i in range(3)] for part in range(2)]

    def save(ref, index, value):
        for part in range(2):
            for i in range(len(value[part])):
                for j in range(3):
                    ref[index, part, i, j] = value[part][i][j]

    def saved(ref, index, rows=3):
        return [[[ref[index, part, i, j] for j in range(3)] for i in range(rows)] for part in range(2)]

    def rolled(m, d, h, part, i, j):
        v = load(m, part, i, j, h)
        if d == 3:
            return jnp.where(g.xcol == NX - 1, g.lanes(v, NX - 1), g.lanes(v, -1))
        if d == 2:
            return g.lanes(v, -NX)
        if d == 1:
            return g.rows(v, -1)
        if h + 1 < halves:
            beyond = g.rows(load(m, part, i, j, h + 1), -depth)
            return jnp.where(g.row >= SUB - depth, beyond, g.rows(v, -depth))
        return g.rows(v, -depth)

    def complete(d, h):
        return d == 3 or (d == 0 and h + 1 < halves)

    slots = {}
    for mu, nu in PLANES:
        for h in range(halves):
            for m, d in ((nu, mu), (mu, nu)):
                slots[m, d, h] = len(slots)
                rows = 3 if complete(d, h) else 2
                save(
                    ahead_s, slots[m, d, h],
                    [[[rolled(m, d, h, part, i, j) for j in range(3)] for i in range(rows)] for part in range(2)],
                )
            save(
                local_s, PLANES.index((mu, nu)) * halves + h,
                product(matrix(mu, h), matrix(nu, h), left_h=True),
            )

    def ahead(m, d, h):
        if complete(d, h):
            return saved(ahead_s, slots[m, d, h])
        index = {c: n for n, c in enumerate(all_comps(d))}

        def get(part, i, j):
            v = ahead_s[slots[m, d, h], part, i, j]
            c = index[(m, part, i, j)]
            if d == 0:
                r = c // g.per * SUB
                edge = g.rows(rt[r : r + SUB, :], SUB - depth - depth * (c % g.per))
                return jnp.where(g.row >= SUB - depth, edge, v)
            if d == 1:
                r = (c // depth * halves + h) * SUB
                edge = g.rows(rz[r : r + SUB, :], depth - 1 - c % depth)
                return jnp.where(g.zrow == depth - 1, edge, v)
            r = (c // g.ygroups * halves + h) * SUB
            edge = g.lanes(ry[r : r + SUB, :], LANES - NX - NX * (c % g.ygroups))
            return jnp.where(g.lane >= LANES - NX, edge, v)

        real = [[get(0, i, j) for j in range(3)] for i in range(2)]
        imag = [[get(1, i, j) for j in range(3)] for i in range(2)]
        third_r, third_i = third_row(real, imag)
        return [real + [third_r], imag + [third_i]]

    seen = set()

    def add(m, c, h, value):
        r = ((m * 8 + c) * halves + h) * SUB
        if (m, c, h) in seen:
            acc[r : r + SUB, :] += value
        else:
            seen.add((m, c, h))
            acc[r : r + SUB, :] = value

    def lower(m, d, h, q):
        base = others(d).index(m) * 8
        if d == 2:
            for c0 in range(0, 8, g.ygroups):
                value = None
                for k in range(g.ygroups):
                    x = g.lanes(q[c0 + k], NX * (k + 1))
                    value = x if value is None else jnp.where(g.lane >= NX * k, x, value)
                r = ((base + c0) // g.ygroups * halves + h) * SUB
                qy[r : r + SUB, :] = value
        elif d == 1:
            for c0 in range(0, 8, depth):
                value = None
                for k in range(depth):
                    x = g.rows(q[c0 + k], k + 1 - depth)
                    value = x if value is None else jnp.where(g.zrow >= k, x, value)
                r = ((base + c0) // depth * halves + h) * SUB
                qz[r : r + SUB, :] = value
        for c in range(8):
            if d == 3:
                add(m, c, h, jnp.where(g.xcol == 0, g.lanes(q[c], 1 - NX), g.lanes(q[c], 1)))
            elif d == 2:
                add(m, c, h, jnp.where(g.lane >= NX, g.lanes(q[c], NX), 0.0))
            elif d == 1:
                add(m, c, h, jnp.where(g.zrow > 0, g.rows(q[c], 1), 0.0))
            else:
                moved = g.rows(q[c], depth)
                add(m, c, h, jnp.where(g.row >= depth, moved, 0.0))
                if h + 1 < halves:
                    add(m, c, h + 1, jnp.where(g.row < depth, moved, 0.0))

    steps = [(pair, h) for pair in PLANES if pair[0] for h in range(halves)]
    steps += [(pair, h) for h in range(halves) for pair in PLANES if not pair[0]]
    arrived, left = set(), {key: halves for key in second}
    for (mu, nu), h in steps:
        n = PLANES.index((mu, nu))
        for d, m in ((mu, nu), (nu, mu)):
            key = (d, None if d == 2 else m)
            if key in first and key not in arrived and not complete(d, h):
                arrived.add(key)
                first[key].wait_recv()
        a = product(ahead(nu, mu, h), ahead(mu, nu, h), right_h=True)
        save(plaq_s, n * halves + h, a)
        b = saved(local_s, n * halves + h)
        lower(mu, nu, h, projected(a, b, left_h=True))
        lower(nu, mu, h, projected(a, b, right_h=True))
        for key in ((mu, nu), (nu, mu)):
            if key in second:
                left[key] -= 1
                if not left[key]:
                    second[key].start()

    for n, (mu, nu) in enumerate(PLANES):
        for h in range(halves):
            e = product(matrix(mu, h), saved(plaq_s, n * halves + h))
            upper = projected(e, matrix(nu, h), right_h=True)
            for c in range(8):
                add(mu, c, h, upper[c])
                add(nu, c, h, -upper[c])

    def complete_rows(get):
        real = [[get(0, i, j) for j in range(3)] for i in range(2)]
        imag = [[get(1, i, j) for j in range(3)] for i in range(2)]
        third_r, third_i = third_row(real, imag)
        return [real + [third_r], imag + [third_i]]

    def behind(m):
        def get(part, i, j):
            c = 12 * m + part * 6 + i * 3 + j
            r = c // g.per * SUB
            return g.rows(br[r : r + SUB, :], -depth * (c % g.per))

        return complete_rows(get)

    def add_faces(m):
        for d in others(m):
            if d in (1, 2):
                second[d, m].wait_recv()
        for h in range(halves):
            for c in range(8):
                r = ((m * 8 + c) * halves + h) * SUB
                value = acc[r : r + SUB, :]
                for d in others(m):
                    b = others(d).index(m) * 8 + c
                    if d == 1:
                        s = (b // depth * halves + h) * SUB
                        x = g.rows(pz[s : s + SUB, :], -(b % depth))
                        value = value + jnp.where(g.zrow == 0, x, 0.0)
                    elif d == 2:
                        s = (b // g.ygroups * halves + h) * SUB
                        x = g.lanes(py[s : s + SUB, :], -NX * (b % g.ygroups))
                        value = value + jnp.where(g.lane < NX, x, 0.0)
                acc[r : r + SUB, :] = value

    for m in (3, 2, 1):
        add_faces(m)

    for key in (("edge", 1), ("edge", 2), 0):
        back[key].wait_recv()
    time_link = behind(0)
    for m in (3, 2, 1):
        back[m].wait_recv()

        def step(part, i, j):
            v = time_link[part][i][j]
            c = part * 6 + i * 3 + j
            if m == 3:
                return jnp.where(g.xcol == NX - 1, g.lanes(v, NX - 1), g.lanes(v, -1))
            if m == 1:
                r = c // SUB * SUB
                edge = g.rows(ezr[r : r + SUB, :], depth - 1 - c % SUB)
                return jnp.where(g.row == depth - 1, edge, g.rows(v, -1))
            r = c // g.ygroups * SUB
            edge = g.lanes(eyr[r : r + SUB, :], LANES - NX - NX * (c % g.ygroups))
            return jnp.where(g.lane >= LANES - NX, edge, g.lanes(v, -NX))

        a = product(matrix(m, 0), complete_rows(step), right_h=True)
        b = product(time_link, behind(m), left_h=True)
        q = projected(a, b, right_h=True)
        for c in range(8):
            add(m, c, 0, jnp.where(g.row < depth, q[c], 0.0))

    add_faces(0)
    for copy in list(first.values()) + list(back.values()) + list(second.values()):
        copy.wait_send()


def expand(halves, acc, hbm, out, sems):
    copies = []
    for m in range(4):
        for h in range(halves):
            rows = [((m * 8 + c) * halves + h) * SUB for c in range(8)]
            f = [acc[r : r + SUB, :] * (COEFF * 0.5 if c < 6 else COEFF) for c, r in enumerate(rows)]

            def put(part, i, j, value):
                out[m, part, i, j, h * SUB : (h + 1) * SUB, :] = value

            for n, (i, j) in enumerate(((0, 1), (0, 2), (1, 2))):
                put(0, i, j, f[n])
                put(0, j, i, -f[n])
                put(1, i, j, f[3 + n])
                put(1, j, i, f[3 + n])
            for i in range(3):
                put(0, i, i, jnp.zeros((SUB, LANES), jnp.float32))
            put(1, 0, 0, f[6])
            put(1, 1, 1, f[7])
            put(1, 2, 2, -(f[6] + f[7]))
        copies.append(pltpu.make_async_copy(out.at[m], hbm.at[m], sems.at[m]))
        copies[-1].start()
    for copy in copies:
        copy.wait()


def per_device(counts, links):
    time_len, depth, flat = links.shape[4:]
    sites = time_len * depth
    assert flat == LANES and SUB % depth == 0 and sites % SUB == 0
    halves = sites // SUB
    rows1, rows2 = sizes(depth, halves)
    vmem = lambda *s: pltpu.VMEM(s + (LANES,), jnp.float32)
    shape = links.shape[:4] + (sites, flat)
    terms = pl.pallas_call(
        functools.partial(force_terms, counts, depth, halves),
        out_shape=pltpu.VMEM((32 * sites, flat), jnp.float32),
        in_specs=[pl.BlockSpec(memory_space=pl.ANY)],
        out_specs=pl.BlockSpec(memory_space=pltpu.VMEM),
        scratch_shapes=[
            vmem(*shape[:-1]),
            vmem(12 * halves, 2, 3, 3, SUB),
            vmem(6 * halves, 2, 3, 3, SUB),
            vmem(6 * halves, 2, 3, 3, SUB),
        ]
        + [vmem(r) for r in rows1 + rows1 + rows2[1:] + rows2[1:]]
        + [vmem(r) for r in (rows1[0] // 3 * 4,) * 2 + (2 * SUB,) * 4]
        + [
            pltpu.SemaphoreType.DMA((5,)),
            pltpu.SemaphoreType.DMA((19,)),
            pltpu.SemaphoreType.DMA((19,)),
        ],
        compiler_params=pltpu.CompilerParams(collective_id=0, has_side_effects=True),
        name="force_terms",
    )(links.reshape(shape))
    out = pl.pallas_call(
        functools.partial(expand, halves),
        out_shape=jax.ShapeDtypeStruct(shape, jnp.float32),
        in_specs=[pl.BlockSpec(memory_space=pltpu.VMEM)],
        out_specs=pl.BlockSpec(memory_space=pl.ANY),
        scratch_shapes=[vmem(*shape[:-1]), pltpu.SemaphoreType.DMA((4,))],
        name="expand",
    )(pltpu.with_memory_space_constraint(terms, pltpu.VMEM))
    return out.reshape(links.shape)


def solution(mesh):
    assert mesh.axis_names == ("gx", "gz", "ta")
    counts = tuple(mesh.shape[a] for a in AXES)
    spec = P(None, None, None, None, "ta", "gz", "gx")
    return jax.shard_map(
        functools.partial(per_device, counts),
        mesh=mesh,
        in_specs=(spec,),
        out_specs=spec,
        check_vma=False,
    )
```
